32 devices in a mesh: row: 4 (over z), col: 8 (over y, x, core).
Axes of the slice: x: 2, y: 2, z: 4, core: 2. Of those that a mesh axis runs over, the one named last changes fastest.
Arguments:
- right_side: float32 [256, 2048], P('row', 'col'), may hold values from -20 to 20
- initial_guess: float32 [256, 2048], P('row', 'col'), may hold values from -3 to 3
- kernel: float32 [31, 31], replicated, may hold values from 0 to 1, as said below
Outputs:
- template: float32 [256, 2048], P('row', 'col')
- residual: float32 [256, 2048], P('row', 'col')
The draws below stay inside these ranges and needn't reach their ends.
Inputs may be any that keep to these rules, and one draw needn't show every extreme that they name: `kernel`: entries are positive and sum to one.
All inputs are finite; a program needn't handle non-finite values.
Results may differ from the reference program's by a relative error of at most 0.0003.
Values sent between devices are 32-bit elements; how exact they have to be, the bound alone decides.
A program may use at most 128 MiB of HBM per device.

```python
import jax
import jax.numpy as jnp

KW = 31
ITERS = 3
NX = 256
NY = 2048


def draw_right_side(key, part):
    rough = jax.random.normal(jax.random.fold_in(key, 11), (NX, NY), jnp.float32)
    column_pos = jnp.arange(NY, dtype=jnp.float32) / max(NY - 1, 1)
    ramp = jnp.exp(jnp.log(3.0) * column_pos)[None, :]
    values = rough * ramp
    return jnp.clip(values, -20.0, 20.0)


def draw_kernel(key, part):
    center = (KW - 1) / 2.0
    offsets = jnp.arange(KW, dtype=jnp.float32) - center
    radius_sq = offsets[:, None] ** 2 + offsets[None, :] ** 2
    profile = jnp.exp(-radius_sq / 98.0)
    factor = jax.random.uniform(jax.random.fold_in(key, 21), (KW, KW), jnp.float32, 0.5, 1.5)
    weights = profile * factor
    return weights / jnp.sum(weights)


def shard_levels(own_key, shape, shards, least, largest):
    def one(position, blocks):
        draws = jax.random.uniform(jax.random.fold_in(jax.random.fold_in(own_key, 6), position), (blocks,), jnp.float32, least / len(shards), largest / len(shards))
        return jnp.repeat(jnp.exp(draws), shape[position] // blocks).reshape((-1,) + (1,) * (len(shape) - position - 1))

    gain = one(*shards[0])
    for cut in shards[1:]:
        gain = gain * one(*cut)
    return gain


def scatter_about(rng, dims, deviation, bound, split=(), kind=jnp.bfloat16):
    level = shard_levels(rng, dims, split, -0.22, 0.18) if split else 1.0
    result = jax.random.normal(rng, dims, jnp.float32) * deviation * level
    return jnp.minimum(jnp.maximum(result, -bound), bound).astype(kind)


def setup_inputs(seed: int = 0) -> dict:
    splits = jax.random.split(jax.random.key(seed), 4)
    return {
        "right_side": draw_right_side(jax.random.fold_in(splits[3], 71), 0),
        "initial_guess": scatter_about(splits[1], (NX, NY), 0.5, 3.0, ((0, 4), (1, 8)), jnp.float32),
        "kernel": draw_kernel(jax.random.fold_in(splits[3], 71), 0),
    }


penalty = 0.05


def convolve(source, taps):
    half_width = taps.shape[0] // 2
    tile_rows, tile_cols = source.shape
    extent = (tile_rows + 2 * half_width, tile_cols + 2 * half_width)
    spectrum = jnp.fft.rfft2(source, s=extent) * jnp.fft.rfft2(taps, s=extent)
    complete = jnp.fft.irfft2(spectrum, s=extent)
    return complete[half_width:half_width + tile_rows, half_width:half_width + tile_cols].astype(source.dtype)


def laplacian(source):
    padded = jnp.pad(source, 1)
    return 4.0 * source - padded[2:, 1:-1] - padded[:-2, 1:-1] - padded[1:-1, 2:] - padded[1:-1, :-2]


def operate(source, kernel):
    blurred = convolve(source, kernel[::-1, ::-1])
    return convolve(blurred, kernel) + penalty * laplacian(source)


def reference(right_side, initial_guess, kernel):
    template = initial_guess
    residual = right_side - operate(template, kernel)
    direction = residual
    norm_now = jnp.sum(residual * residual)
    for iteration in range(ITERS):
        applied = operate(direction, kernel)
        step_size = norm_now / jnp.sum(direction * applied)
        template = template + step_size * direction
        residual = residual - step_size * applied
        norm_next = jnp.sum(residual * residual)
        direction = residual + (norm_next / norm_now) * direction
        norm_now = norm_next
    return template, residual
```

```python
import functools

import jax
import jax.numpy as jnp
from jax import lax
from jax.experimental import pallas as pl
from jax.experimental.pallas import tpu as pltpu
from jax.sharding import PartitionSpec as P

PENALTY = 0.05
LANES = 128
MESH = pl.DeviceIdType.MESH
DIRECTIONS = ((-1, 0), (1, 0), (-1, -1), (-1, 1), (1, -1), (1, 1), (0, -1), (0, 1))
MOMENTS = 6


def split(x):
    high = x.astype(jnp.bfloat16)
    low = (x - high.astype(jnp.float32)).astype(jnp.bfloat16)
    return high, low


def body(
    n_row, n_col,
    right_hbm, guess_hbm, kernel_hbm, template_ref, residual_ref,
    right_ref, guess_ref, kernel_ref, packed, packed_right, lines_ref, table, high_ref, low_ref,
    wide0, wide1, partial_ref, block_ref, state_ref, basis_ref, red,
    load_sem, send_sem, recv_sem, red_send, red_recv,
):
    rows, cols = right_ref.shape
    row, col = lax.axis_index("row"), lax.axis_index("col")
    me, count = row * n_col + col, n_row * n_col
    width = kernel_ref.shape[0]
    blk = rows // 2
    edge = rows
    total = cols + 2 * edge
    groups, own_g, edge_g = total // 16, cols // 16, edge // 16

    barrier = pltpu.get_barrier_semaphore()

    def others(act):
        def along_row(r, carry):
            def one(c, inner):
                pl.when(r * n_col + c != me)(lambda: act((r, c)))
                return inner

            return lax.fori_loop(0, n_col, one, carry)

        lax.fori_loop(0, n_row, along_row, 0)

    others(
        lambda place: pl.semaphore_signal(barrier, inc=1, device_id=place, device_id_type=MESH)
    )
    loads = [
        pltpu.make_async_copy(src, dst, load_sem.at[k])
        for k, (src, dst) in enumerate(
            ((kernel_hbm, kernel_ref), (guess_hbm, guess_ref), (right_hbm, right_ref))
        )
    ]
    for load in loads:
        load.start()

    lane = lax.broadcasted_iota(jnp.int32, (8, LANES), 1)
    lane1 = lane[0:1]

    def low_half(shape):
        return lax.broadcasted_iota(jnp.int32, shape, len(shape) - 1) < LANES // 2

    def quarters(a, b, c, d):
        q = lax.broadcasted_iota(jnp.int32, a.shape, 1)
        return jnp.where(
            q < 2 * blk, jnp.where(q < blk, a, b), jnp.where(q < 3 * blk, c, d)
        )

    def inside(dr, dc):
        checks = []
        if dr:
            checks.append(row + dr >= 0 if dr < 0 else row + dr < n_row)
        if dc:
            checks.append(col + dc >= 0 if dc < 0 else col + dc < n_col)
        return functools.reduce(jnp.logical_and, checks)

    def clear(buf, lead):
        zero_tall = jnp.zeros(lead + (1, groups, 8, LANES), jnp.float32)
        zero_edge = jnp.zeros(lead + (3, edge_g, 8, LANES), jnp.float32)
        at = (slice(None),) * len(lead)

        @pl.when(row == 0)
        def _():
            buf[at + (slice(0, 1),)] = zero_tall

        @pl.when(row == n_row - 1)
        def _():
            buf[at + (slice(2, 3),)] = zero_tall

        @pl.when(col == 0)
        def _():
            buf[at + (slice(None), slice(0, edge_g))] = zero_edge

        @pl.when(col == n_col - 1)
        def _():
            buf[at + (slice(None), slice(groups - edge_g, groups))] = zero_edge

    clear(packed, (2,))
    clear(packed_right, (1,))

    def flip(x):
        return jnp.concatenate([x[a : a + 1] for a in reversed(range(width))] + [x[width:]], axis=0)

    def build_tables():
        taps = kernel_ref[...]
        taps = jnp.concatenate([taps, jnp.zeros((width, LANES - width), jnp.float32)], axis=1)
        taps = jnp.concatenate([taps, jnp.zeros((LANES - width, LANES), jnp.float32)], axis=0)
        lines_ref[0] = pltpu.roll(flip(taps).T, LANES - width, axis=1)
        lines_ref[1] = pltpu.roll(taps.T, LANES - width, axis=1)

        for which in range(2):
            for q in range(2):
                for h in range(2):
                    for half in range(2):
                        lines = []
                        for g in range(4):
                            b = 16 * q + 8 * h + 4 * half + g
                            source = b - 1 if which == 0 else width - b
                            if b == 0:
                                lines.append(jnp.zeros((8, LANES), jnp.float32))
                            else:
                                lines.append(
                                    jnp.broadcast_to(lines_ref[which, source : source + 1, :], (8, LANES))
                                )
                        tiles = []
                        for k in range(2 * blk // 8):
                            pieces = [
                                pltpu.roll(
                                    lines[g], (blk * g + 8 * k) % LANES, axis=1, stride=1, stride_axis=0
                                )
                                for g in range(4)
                            ]
                            tiles.append(quarters(*pieces))
                        high, low = split(jnp.concatenate(tiles, axis=0))
                        at_row = pl.ds(LANES * q + 2 * blk * h, 2 * blk)
                        at_lane = pl.ds(LANES * half, LANES)
                        table[which, 0, at_row, at_lane] = high
                        table[which, 1, at_row, at_lane] = low

    def pack(tile):
        tall = jnp.concatenate([tile, pltpu.roll(tile, cols - 8, axis=1)], axis=0)
        pieces = [tall[:, k : k + LANES].T for k in range(0, cols, LANES)]
        form = jnp.concatenate(pieces, axis=0)
        return form.reshape(own_g, 2, 8, LANES)[:, 0]

    def expand(pk):
        after = jnp.concatenate([pk[1:], pk[:1]], axis=0)
        odd = jnp.where(low_half(pk.shape), after, pk).reshape(-1, LANES)
        odd = pltpu.roll(odd, LANES // 2, axis=1).reshape(pk.shape)
        return jnp.stack([pk, odd], axis=1).reshape(pk.shape[0] * 16, LANES)

    def strip(buf, sems, phase, index):
        dr, dc = DIRECTIONS[index]
        dst_strip = 1 - dr
        c_src, c_dst, c_len = (
            (edge_g, groups - edge_g, edge_g) if dc < 0
            else (groups - 2 * edge_g, 0, edge_g) if dc > 0
            else (edge_g, edge_g, own_g)
        )
        return pltpu.make_async_remote_copy(
            src_ref=buf.at[phase, 1, pl.ds(c_src, c_len)],
            dst_ref=buf.at[phase, 1 - (-dr), pl.ds(c_dst, c_len)] if False else buf.at[phase, dst_strip, pl.ds(c_dst, c_len)],
            send_sem=send_sem.at[sems, index],
            recv_sem=recv_sem.at[sems, index],
            device_id=(row + dr, col + dc),
            device_id_type=MESH,
        )

    def each(buf, sems, phase, act, sign):
        for index, (dr, dc) in enumerate(DIRECTIONS):
            pl.when(inside(sign * dr, sign * dc))(
                lambda index=index: act(strip(buf, sems, phase, index))
            )

    def send(buf, sems, phase):
        each(buf, sems, phase, lambda c: c.start(), 1)

    def receive(buf, sems, phase):
        each(buf, sems, phase, lambda c: c.wait_recv(), -1)

    def finish(buf, sems, phase):
        each(buf, sems, phase, lambda c: c.wait_send(), 1)

    first_row, last_row = row == 0, row == n_row - 1
    left_on = jnp.where(col == 0, 0.0, 1.0)
    right_on = jnp.where(col == n_col - 1, 0.0, 1.0)

    def row_mask(start):
        at = start + lax.rem(lane1, blk)
        off = jnp.logical_or(
            jnp.logical_and(at < 0, first_row), jnp.logical_and(at >= rows, last_row)
        )
        return jnp.where(off, 0.0, 1.0)

    def put_block(k, start, value, margin):
        if start < 0 or start + blk > rows:
            value = value * row_mask(start)
        n = value.shape[0]
        if margin:
            block_ref[k, 0:margin, :] = value[0:margin] * left_on
            block_ref[k, margin : n - margin, :] = value[margin : n - margin]
            block_ref[k, n - margin : n, :] = value[n - margin : n] * right_on
        else:
            block_ref[k, 0:n, :] = value

    def load_windows(n, n_in):
        for k in range(n):
            low_cols = [block_ref[k + j, 0:n_in, :] for j in range(2)]
            high_cols = [block_ref[k + j, 8 : n_in + 8, :] for j in range(2)]
            put_window(k, n_in, quarters(low_cols[0], low_cols[1], high_cols[0], high_cols[1]))

    def put_window(k, n_in, value):
        high, low = split(value)
        high_ref[k * n_in : (k + 1) * n_in, :] = high
        low_ref[k * n_in : (k + 1) * n_in, :] = low

    def convolve(which, n, n_in):
        m = n * n_in
        lhs = jnp.concatenate(
            [high_ref[0:m, :], high_ref[16 : m + 16, :], low_ref[0:m, :], low_ref[16 : m + 16, :],
             high_ref[0:m, :], high_ref[16 : m + 16, :]],
            axis=1,
        )
        rhs = jnp.concatenate([table[which, 0], table[which, 0], table[which, 1]], axis=0)
        out = jnp.dot(lhs, rhs, preferred_element_type=jnp.float32)
        wide0[0:m, :] = out[:, 0:LANES]
        wide1[0:m, :] = out[:, LANES:]

    def assemble(k, n_in):
        n_out = n_in - 2 * 16
        base = k * n_in
        partial_ref[0 : n_out + 8, :] = (
            wide0[base : base + n_out + 8, :] + wide1[base + 4 : base + n_out + 12, :]
        )
        total_ = quarters(*(partial_ref[j : j + n_out, :] for j in range(4)))
        total_ = total_ + pltpu.roll(total_, 2 * blk, axis=1)
        return total_ + pltpu.roll(total_, blk, axis=1)

    def window_sources(phase):
        up, mid, down = (expand(packed[phase, s]) for s in range(3))
        odd = lax.rem(lax.broadcasted_iota(jnp.int32, mid.shape, 1) // blk, 2) == 1
        upper = jnp.where(odd, pltpu.roll(mid, blk, axis=1), pltpu.roll(up, LANES - blk, axis=1))
        lower = jnp.where(odd, pltpu.roll(down, blk, axis=1), pltpu.roll(mid, LANES - blk, axis=1))
        natural = jnp.where(low_half(mid.shape), upper, pltpu.roll(lower, LANES // 2, axis=1))
        return (up, upper, mid, lower, down), natural

    def smooth(index, n_out):
        start = (total - n_out) // 2
        if index == 1:
            start = 16
        center = state_ref[index, start : start + n_out, :]
        left = state_ref[index, start - 1 : start - 1 + n_out, :]
        right = state_ref[index, start + 1 : start + 1 + n_out, :]
        upper = pltpu.roll(center, 1, axis=1)
        lower = pltpu.roll(center, LANES - 1, axis=1)
        return PENALTY * (4.0 * center - upper - lower - left - right)

    def merge(n):
        return quarters(*(block_ref[k, 0:n, :] for k in range(4)))

    def row_sum(x):
        return jnp.sum(x, axis=0, keepdims=True)

    own_lanes = jnp.logical_and(lane1 >= blk, lane1 < 3 * blk)

    def own(x):
        return jnp.where(own_lanes, x, 0.0)

    def first_half(phase):
        windows, natural = window_sources(phase)
        state_ref[0] = natural
        for k, w in enumerate(windows):
            put_window(k, total, w)
        convolve(0, 5, total)
        for k in range(5):
            put_block(k, -blk - 16 + blk * k, assemble(k, total), 48)
        load_windows(4, total - 32)
        convolve(1, 4, total - 32)
        for k in range(4):
            put_block(k, -blk + blk * k, assemble(k, total - 32), 32)

    def second_half_a():
        n_in = total - 64
        load_windows(3, n_in)
        convolve(0, 3, n_in)
        for k in range(3):
            put_block(k, -16 + blk * k, assemble(k, n_in), 16)

    def second_half_b():
        n_in = total - 96
        load_windows(2, n_in)
        convolve(1, 2, n_in)
        for k in range(2):
            block_ref[k, 0 : n_in - 32, :] = assemble(k, n_in)

    def masked_natural(value):
        at = lane1 - blk
        off = jnp.logical_or(
            jnp.logical_and(at < 0, first_row), jnp.logical_and(at >= rows, last_row)
        )
        value = value * jnp.where(off, 0.0, 1.0)
        n = value.shape[0]
        return jnp.concatenate(
            [value[0:32] * left_on, value[32 : n - 32], value[n - 32 :] * right_on], axis=0
        )

    def spill_natural(value):
        n = value.shape[0]
        turned = [value] + [pltpu.roll(value, LANES - blk * j, axis=1) for j in range(1, 4)]
        del n
        return turned

    def windows_from_natural(value):
        n = value.shape[0]
        after = jnp.concatenate([value[8:], value[:8]], axis=0)
        mask = low_half(value.shape)
        put_window(0, n, jnp.where(mask, value, pltpu.roll(after, LANES // 2, axis=1)))
        put_window(
            1, n,
            jnp.where(mask, pltpu.roll(value, LANES - blk, axis=1), pltpu.roll(after, blk, axis=1)),
        )
        put_window(2, n, jnp.where(mask, pltpu.roll(value, LANES // 2, axis=1), after))

    def finish_pair(index):
        parts = block_ref[0, 0:cols, :], block_ref[1, 0:cols, :]
        both = quarters(parts[0], parts[0], parts[1], parts[1])
        out = own(both + smooth_own())
        basis_ref[index] = out
        return out

    def smooth_own():
        start = 32
        center = state_ref[1, start : start + cols, :]
        left = state_ref[1, start - 1 : start - 1 + cols, :]
        right = state_ref[1, start + 1 : start + 1 + cols, :]
        upper = pltpu.roll(center, 1, axis=1)
        lower = pltpu.roll(center, LANES - 1, axis=1)
        return PENALTY * (4.0 * center - upper - lower - left - right)

    def smooth_wide():
        n_out = total - 64
        start = 32
        center = state_ref[0, start : start + n_out, :]
        left = state_ref[0, start - 1 : start - 1 + n_out, :]
        right = state_ref[0, start + 1 : start + 1 + n_out, :]
        upper = pltpu.roll(center, 1, axis=1)
        lower = pltpu.roll(center, LANES - 1, axis=1)
        return PENALTY * (4.0 * center - upper - lower - left - right)

    loads[0].wait()
    build_tables()
    loads[1].wait()
    packed[0, 1, edge_g : edge_g + own_g] = pack(guess_ref[...])
    loads[2].wait()
    packed_right[0, 1, edge_g : edge_g + own_g] = pack(right_ref[...])
    pl.semaphore_wait(barrier, count - 1)
    send(packed, 0, 0)
    send(packed_right, 1, 0)

    n_mid = total - 64
    receive(packed, 0, 0)
    first_half(0)
    receive(packed_right, 1, 0)
    up_r, mid_r, down_r = (expand(packed_right[0, s]) for s in range(3))
    sl = slice(32, 32 + n_mid)
    nat_r = jnp.where(
        low_half((n_mid, LANES)),
        jnp.where(
            lax.broadcasted_iota(jnp.int32, (n_mid, LANES), 1) < blk,
            pltpu.roll(up_r[sl], LANES - blk, axis=1),
            pltpu.roll(mid_r[sl], blk, axis=1),
        ),
        jnp.where(
            lax.broadcasted_iota(jnp.int32, (n_mid, LANES), 1) < 3 * blk,
            pltpu.roll(mid_r[sl], blk, axis=1),
            pltpu.roll(down_r[sl], 3 * blk, axis=1),
        ),
    )
    start_residual = masked_natural(nat_r - (merge(n_mid) + smooth_wide()))
    state_ref[1, 0:n_mid, :] = start_residual
    basis_ref[3] = own(state_ref[0, edge : edge + cols, :])
    r0 = own(start_residual[32 : 32 + cols])
    basis_ref[0] = r0
    windows_from_natural(start_residual)
    convolve(0, 3, n_mid)
    for k in range(3):
        put_block(k, -16 + blk * k, assemble(k, n_mid), 16)
    second_half_b()
    w1 = finish_pair(1)
    turned = pltpu.roll(w1, LANES - blk, axis=1).reshape(own_g, 2, 8, LANES)
    turned_up = pltpu.roll(w1, blk, axis=1).reshape(own_g, 2, 8, LANES)
    pk = jnp.where(low_half((own_g, 8, LANES)), turned[:, 0], turned_up[:, 1])
    packed[1, 1, edge_g : edge_g + own_g] = pk
    send(packed, 2, 1)
    finish(packed, 0, 0)
    finish(packed_right, 1, 0)
    m0, m1, m2 = row_sum(r0 * r0), row_sum(r0 * w1), row_sum(w1 * w1)

    receive(packed, 2, 1)
    first_half(1)
    second = masked_natural(merge(n_mid) + smooth_wide())
    state_ref[1, 0:n_mid, :] = second
    w2 = own(second[32 : 32 + cols])
    basis_ref[2] = w2
    m3, m4 = row_sum(basis_ref[1] * w2), row_sum(w2 * w2)
    windows_from_natural(second)
    convolve(0, 3, n_mid)
    for k in range(3):
        put_block(k, -16 + blk * k, assemble(k, n_mid), 16)
    k_rows = [block_ref[k, 16 : 16 + cols, :] for k in range(3)]
    joined = quarters(k_rows[0], k_rows[1], k_rows[2], k_rows[2])
    inside_k = jnp.logical_and(lane1 >= 16, lane1 < 16 + rows)
    joined = jnp.where(inside_k, joined, 0.0)
    smooth2 = smooth_own()
    m5 = row_sum(joined * joined) + row_sum(w2 * smooth2)

    def fold(x):
        for k in (64, 32, 16):
            x = x + pltpu.roll(x, k, axis=1)
        return x

    line = jnp.zeros((1, LANES), jnp.float32)
    for k, m in enumerate((m0, m1, m2, m3, m4, m5)):
        at_k = jnp.logical_and(lane1 >= 16 * k, lane1 < 16 * (k + 1))
        line = jnp.where(at_k, fold(m), line)
    red[me] = line

    def red_copy(place):
        return pltpu.make_async_remote_copy(
            src_ref=red.at[me], dst_ref=red.at[me], send_sem=red_send.at[0], recv_sem=red_recv.at[0],
            device_id=place, device_id_type=MESH,
        )

    all_red = pltpu.make_async_remote_copy(
        src_ref=red.at[pl.ds(0, count - 1)], dst_ref=red.at[pl.ds(0, count - 1)],
        send_sem=red_send.at[0], recv_sem=red_recv.at[0],
        device_id=(row, col), device_id_type=MESH,
    )
    others(lambda place: red_copy(place).start())
    finish(packed, 2, 1)
    second_half_b()
    w3 = finish_pair(4)

    all_red.wait_recv()
    sums = jnp.sum(red[...], axis=0)
    m = [
        jnp.sum(
            jnp.where(jnp.logical_and(lane1 >= 16 * k, lane1 < 16 * (k + 1)), sums, 0.0),
            axis=1, keepdims=True,
        )
        for k in range(MOMENTS)
    ]

    def times(p, q):
        return sum(
            p[i] * q[j] * m[i + j] for i in range(len(p)) for j in range(len(q))
        )

    rho, pi = [jnp.ones((1, 1), jnp.float32)], [jnp.ones((1, 1), jnp.float32)]
    step_sum = []
    norm = m[0]
    for it in range(3):
        shifted = [jnp.zeros((1, 1), jnp.float32)] + pi
        alpha = norm / times(pi, shifted)
        step_sum = [
            (step_sum[i] if i < len(step_sum) else 0.0) + alpha * pi[i] for i in range(len(pi))
        ]
        rho = [
            (rho[i] if i < len(rho) else 0.0) - alpha * shifted[i] for i in range(len(shifted))
        ]
        if it < 2:
            norm_next = times(rho, rho)
            beta = norm_next / norm
            pi = [rho[i] + (beta * pi[i] if i < len(pi) else 0.0) for i in range(len(rho))]
            norm = norm_next

    r0, w1, w2 = basis_ref[0], basis_ref[1], basis_ref[2]
    template = basis_ref[3] + step_sum[0] * r0 + step_sum[1] * w1 + step_sum[2] * w2
    residual = rho[0] * r0 + rho[1] * w1 + rho[2] * w2 + rho[3] * w3
    for ref, value in ((template_ref, template), (residual_ref, residual)):
        for k in range(0, cols, LANES):
            ref[:, k : k + LANES] = value[k : k + LANES].T[blk : blk + rows]
    all_red.wait_send()


def on_device(n_row, n_col, right_side, initial_guess, kernel):
    rows, cols = right_side.shape
    total = cols + 2 * rows
    count = n_row * n_col
    shape = jax.ShapeDtypeStruct((rows, cols), jnp.float32)
    f32, bf16 = jnp.float32, jnp.bfloat16
    copies = len(DIRECTIONS)
    return pl.pallas_call(
        functools.partial(body, n_row, n_col),
        out_shape=(shape, shape),
        in_specs=[pl.BlockSpec(memory_space=pl.ANY)] * 3,
        out_specs=[pl.BlockSpec(memory_space=pltpu.VMEM)] * 2,
        scratch_shapes=[
            pltpu.VMEM((rows, cols), f32),
            pltpu.VMEM((rows, cols), f32),
            pltpu.VMEM(kernel.shape, f32),
            pltpu.VMEM((2, 3, total // 16, 8, LANES), f32),
            pltpu.VMEM((1, 3, total // 16, 8, LANES), f32),
            pltpu.VMEM((2, LANES, LANES), f32),
            pltpu.VMEM((2, 2, 2 * LANES, 2 * LANES), bf16),
            pltpu.VMEM((5 * total + 16, LANES), bf16),
            pltpu.VMEM((5 * total + 16, LANES), bf16),
            pltpu.VMEM((5 * total + 16, LANES), f32),
            pltpu.VMEM((5 * total + 16, LANES), f32),
            pltpu.VMEM((total, LANES), f32),
            pltpu.VMEM((5, total + 8, LANES), f32),
            pltpu.VMEM((2, total, LANES), f32),
            pltpu.VMEM((5, cols, LANES), f32),
            pltpu.VMEM((count, 1, LANES), f32),
            pltpu.SemaphoreType.DMA((3,)),
            pltpu.SemaphoreType.DMA((3, copies)),
            pltpu.SemaphoreType.DMA((3, copies)),
            pltpu.SemaphoreType.DMA((1,)),
            pltpu.SemaphoreType.DMA((1,)),
        ],
        compiler_params=pltpu.CompilerParams(collective_id=0, has_side_effects=True),
    )(right_side, initial_guess, kernel)


def solution(mesh):
    placed = (P("row", "col"), P("row", "col"), P())
    return jax.shard_map(
        functools.partial(on_device, mesh.shape["row"], mesh.shape["col"]),
        mesh=mesh,
        in_specs=placed,
        out_specs=(P("row", "col"), P("row", "col")),
        check_vma=False,
    )
```

```python
import functools

import jax
import jax.numpy as jnp
from jax import lax
from jax.experimental import pallas as pl
from jax.experimental.pallas import tpu as pltpu
from jax.sharding import PartitionSpec as P

PENALTY = 0.05
LANES = 128
MESH = pl.DeviceIdType.MESH
DIRECTIONS = ((-1, 0), (1, 0), (-1, -1), (-1, 1), (1, -1), (1, 1), (0, -1), (0, 1))
MOMENTS = 6


def split(x):
    high = x.astype(jnp.bfloat16)
    low = (x - high.astype(jnp.float32)).astype(jnp.bfloat16)
    return high, low


def body(n_row, n_col, *refs):
    pieces = [pltpu.ACC(unit)((16, 256), jnp.float32) for unit in range(2) for _ in range(64)]

    def inner(*accs):
        run(n_row, n_col, (accs[:64], accs[64:]), *refs)

    pl.run_scoped(inner, *pieces)


def run(
    n_row, n_col, accs,
    right_hbm, guess_hbm, kernel_hbm, template_ref, residual_ref,
    right_ref, guess_ref, kernel_ref, packed, packed_right, lines_ref, table, high_ref, low_ref,
    wide0, wide1, partial_ref, block_ref, state_ref, basis_ref, red,
    load_sem, send_sem, recv_sem, red_send, red_recv,
):
    rows, cols = right_ref.shape
    row, col = lax.axis_index("row"), lax.axis_index("col")
    me, count = row * n_col + col, n_row * n_col
    width = kernel_ref.shape[0]
    blk = rows // 2
    edge = rows
    total = cols + 2 * edge
    groups, own_g, edge_g = total // 16, cols // 16, edge // 16

    barrier = pltpu.get_barrier_semaphore()

    def others(act):
        def along_row(r, carry):
            def one(c, inner):
                pl.when(r * n_col + c != me)(lambda: act((r, c)))
                return inner

            return lax.fori_loop(0, n_col, one, carry)

        lax.fori_loop(0, n_row, along_row, 0)

    others(
        lambda place: pl.semaphore_signal(barrier, inc=1, device_id=place, device_id_type=MESH)
    )
    loads = [
        pltpu.make_async_copy(src, dst, load_sem.at[k])
        for k, (src, dst) in enumerate(
            ((kernel_hbm, kernel_ref), (guess_hbm, guess_ref), (right_hbm, right_ref))
        )
    ]
    for load in loads:
        load.start()

    lane = lax.broadcasted_iota(jnp.int32, (8, LANES), 1)
    lane1 = lane[0:1]

    def low_half(shape):
        return lax.broadcasted_iota(jnp.int32, shape, len(shape) - 1) < LANES // 2

    def quarters(a, b, c, d):
        q = lax.broadcasted_iota(jnp.int32, a.shape, 1)
        return jnp.where(
            q < 2 * blk, jnp.where(q < blk, a, b), jnp.where(q < 3 * blk, c, d)
        )

    def inside(dr, dc):
        checks = []
        if dr:
            checks.append(row + dr >= 0 if dr < 0 else row + dr < n_row)
        if dc:
            checks.append(col + dc >= 0 if dc < 0 else col + dc < n_col)
        return functools.reduce(jnp.logical_and, checks)

    def clear(buf, lead):
        zero_tall = jnp.zeros(lead + (1, groups, 8, LANES), jnp.float32)
        zero_edge = jnp.zeros(lead + (3, edge_g, 8, LANES), jnp.float32)
        at = (slice(None),) * len(lead)

        @pl.when(row == 0)
        def _():
            buf[at + (slice(0, 1),)] = zero_tall

        @pl.when(row == n_row - 1)
        def _():
            buf[at + (slice(2, 3),)] = zero_tall

        @pl.when(col == 0)
        def _():
            buf[at + (slice(None), slice(0, edge_g))] = zero_edge

        @pl.when(col == n_col - 1)
        def _():
            buf[at + (slice(None), slice(groups - edge_g, groups))] = zero_edge

    clear(packed, (2,))
    clear(packed_right, (1,))

    def flip(x):
        return jnp.concatenate([x[a : a + 1] for a in reversed(range(width))] + [x[width:]], axis=0)

    def build_tables():
        taps = kernel_ref[...]
        taps = jnp.concatenate([taps, jnp.zeros((width, LANES - width), jnp.float32)], axis=1)
        taps = jnp.concatenate([taps, jnp.zeros((LANES - width, LANES), jnp.float32)], axis=0)
        lines_ref[0] = pltpu.roll(flip(taps).T, LANES - width, axis=1)
        lines_ref[1] = pltpu.roll(taps.T, LANES - width, axis=1)

        for which in range(2):
            for q in range(2):
                for h in range(2):
                    for half in range(2):
                        lines = []
                        for g in range(4):
                            b = 16 * q + 8 * h + 4 * half + g
                            source = b - 1 if which == 0 else width - b
                            if b == 0:
                                lines.append(jnp.zeros((8, LANES), jnp.float32))
                            else:
                                lines.append(
                                    jnp.broadcast_to(lines_ref[which, source : source + 1, :], (8, LANES))
                                )
                        tiles = []
                        for k in range(2 * blk // 8):
                            pieces = [
                                pltpu.roll(
                                    lines[g], (blk * g + 8 * k) % LANES, axis=1, stride=1, stride_axis=0
                                )
                                for g in range(4)
                            ]
                            tiles.append(quarters(*pieces))
                        high, low = split(jnp.concatenate(tiles, axis=0))
                        at_row = pl.ds(LANES * q + 2 * blk * h, 2 * blk)
                        at_lane = pl.ds(LANES * half, LANES)
                        table[which, 0, at_row, at_lane] = high
                        table[which, 1, at_row, at_lane] = low

    def pack(tile):
        tall = jnp.concatenate([tile, pltpu.roll(tile, cols - 8, axis=1)], axis=0)
        pieces = [tall[:, k : k + LANES].T for k in range(0, cols, LANES)]
        form = jnp.concatenate(pieces, axis=0)
        return form.reshape(own_g, 2, 8, LANES)[:, 0]

    def expand(pk):
        after = jnp.concatenate([pk[1:], pk[:1]], axis=0)
        odd = jnp.where(low_half(pk.shape), after, pk).reshape(-1, LANES)
        odd = pltpu.roll(odd, LANES // 2, axis=1).reshape(pk.shape)
        return jnp.stack([pk, odd], axis=1).reshape(pk.shape[0] * 16, LANES)

    def strip(buf, sems, phase, index):
        dr, dc = DIRECTIONS[index]
        dst_strip = 1 - dr
        c_src, c_dst, c_len = (
            (edge_g, groups - edge_g, edge_g) if dc < 0
            else (groups - 2 * edge_g, 0, edge_g) if dc > 0
            else (edge_g, edge_g, own_g)
        )
        return pltpu.make_async_remote_copy(
            src_ref=buf.at[phase, 1, pl.ds(c_src, c_len)],
            dst_ref=buf.at[phase, 1 - (-dr), pl.ds(c_dst, c_len)] if False else buf.at[phase, dst_strip, pl.ds(c_dst, c_len)],
            send_sem=send_sem.at[sems, index],
            recv_sem=recv_sem.at[sems, index],
            device_id=(row + dr, col + dc),
            device_id_type=MESH,
        )

    def each(buf, sems, phase, act, sign):
        for index, (dr, dc) in enumerate(DIRECTIONS):
            pl.when(inside(sign * dr, sign * dc))(
                lambda index=index: act(strip(buf, sems, phase, index))
            )

    def send(buf, sems, phase):
        each(buf, sems, phase, lambda c: c.start(), 1)

    def receive(buf, sems, phase):
        each(buf, sems, phase, lambda c: c.wait_recv(), -1)

    def finish(buf, sems, phase):
        each(buf, sems, phase, lambda c: c.wait_send(), 1)

    first_row, last_row = row == 0, row == n_row - 1
    left_on = jnp.where(col == 0, 0.0, 1.0)
    right_on = jnp.where(col == n_col - 1, 0.0, 1.0)

    def row_mask(start):
        at = start + lax.rem(lane1, blk)
        off = jnp.logical_or(
            jnp.logical_and(at < 0, first_row), jnp.logical_and(at >= rows, last_row)
        )
        return jnp.where(off, 0.0, 1.0)

    def put_block(k, start, value, margin):
        if start < 0 or start + blk > rows:
            value = value * row_mask(start)
        n = value.shape[0]
        if margin:
            block_ref[k, 0:margin, :] = value[0:margin] * left_on
            block_ref[k, margin : n - margin, :] = value[margin : n - margin]
            block_ref[k, n - margin : n, :] = value[n - margin : n] * right_on
        else:
            block_ref[k, 0:n, :] = value

    def load_windows(n, n_in):
        for k in range(n):
            low_cols = [block_ref[k + j, 0:n_in, :] for j in range(2)]
            high_cols = [block_ref[k + j, 8 : n_in + 8, :] for j in range(2)]
            put_window(k, n_in, quarters(low_cols[0], low_cols[1], high_cols[0], high_cols[1]))

    def put_window(k, n_in, value):
        high, low = split(value)
        high_ref[k * n_in : (k + 1) * n_in, :] = high
        low_ref[k * n_in : (k + 1) * n_in, :] = low

    next_piece = [0, 0]

    def take(unit):
        acc = accs[unit][next_piece[unit] % len(accs[unit])]
        next_piece[unit] += 1
        return acc

    def convolve(which, n, n_in):
        units = (n_in - 16) // 16
        for k in range(n):
            cut = (units + 1 - k % 2) // 2
            share = (range(0, cut), range(cut, units))
            held = [[take(unit) for _ in share[unit]] for unit in range(2)]
            for part in range(2):
                for unit in range(2):
                    pltpu.matmul_push_rhs(table[which, part], staging_register=part, mxu_index=unit)
            for source, load in ((high_ref, 0), (low_ref, None), (high_ref, 1)):
                for unit in range(2):
                    for i, (u, acc) in enumerate(zip(share[unit], held[unit])):
                        at = k * n_in + 16 * u
                        lhs = jnp.concatenate([source[at : at + 16, :], source[at + 16 : at + 32, :]], axis=1)
                        pltpu.matmul_acc_lhs(acc, lhs, load_staged_rhs=load if i == 0 else None)
            for unit in range(2):
                for u, acc in zip(share[unit], held[unit]):
                    out = pltpu.matmul_pop(acc)
                    at = k * n_in + 16 * u
                    wide0[at : at + 16, :] = out[:, 0:LANES]
                    wide1[at : at + 16, :] = out[:, LANES:]

    def assemble(k, n_in):
        n_out = n_in - 2 * 16
        base = k * n_in
        partial_ref[0 : n_out + 8, :] = (
            wide0[base : base + n_out + 8, :] + wide1[base + 4 : base + n_out + 12, :]
        )
        total_ = quarters(*(partial_ref[j : j + n_out, :] for j in range(4)))
        total_ = total_ + pltpu.roll(total_, 2 * blk, axis=1)
        return total_ + pltpu.roll(total_, blk, axis=1)

    def window_sources(phase):
        up, mid, down = (expand(packed[phase, s]) for s in range(3))
        odd = lax.rem(lax.broadcasted_iota(jnp.int32, mid.shape, 1) // blk, 2) == 1
        upper = jnp.where(odd, pltpu.roll(mid, blk, axis=1), pltpu.roll(up, LANES - blk, axis=1))
        lower = jnp.where(odd, pltpu.roll(down, blk, axis=1), pltpu.roll(mid, LANES - blk, axis=1))
        natural = jnp.where(low_half(mid.shape), upper, pltpu.roll(lower, LANES // 2, axis=1))
        return (up, upper, mid, lower, down), natural

    def smooth(index, n_out):
        start = (total - n_out) // 2
        if index == 1:
            start = 16
        center = state_ref[index, start : start + n_out, :]
        left = state_ref[index, start - 1 : start - 1 + n_out, :]
        right = state_ref[index, start + 1 : start + 1 + n_out, :]
        upper = pltpu.roll(center, 1, axis=1)
        lower = pltpu.roll(center, LANES - 1, axis=1)
        return PENALTY * (4.0 * center - upper - lower - left - right)

    def merge(n):
        return quarters(*(block_ref[k, 0:n, :] for k in range(4)))

    def row_sum(x):
        return jnp.sum(x, axis=0, keepdims=True)

    own_lanes = jnp.logical_and(lane1 >= blk, lane1 < 3 * blk)

    def own(x):
        return jnp.where(own_lanes, x, 0.0)

    def first_half(phase):
        windows, natural = window_sources(phase)
        state_ref[0] = natural
        for k, w in enumerate(windows):
            put_window(k, total, w)
        convolve(0, 5, total)
        for k in range(5):
            put_block(k, -blk - 16 + blk * k, assemble(k, total), 48)
        load_windows(4, total - 32)
        convolve(1, 4, total - 32)
        for k in range(4):
            put_block(k, -blk + blk * k, assemble(k, total - 32), 32)

    def second_half_a():
        n_in = total - 64
        load_windows(3, n_in)
        convolve(0, 3, n_in)
        for k in range(3):
            put_block(k, -16 + blk * k, assemble(k, n_in), 16)

    def second_half_b():
        n_in = total - 96
        load_windows(2, n_in)
        convolve(1, 2, n_in)
        for k in range(2):
            block_ref[k, 0 : n_in - 32, :] = assemble(k, n_in)

    def masked_natural(value):
        at = lane1 - blk
        off = jnp.logical_or(
            jnp.logical_and(at < 0, first_row), jnp.logical_and(at >= rows, last_row)
        )
        value = value * jnp.where(off, 0.0, 1.0)
        n = value.shape[0]
        return jnp.concatenate(
            [value[0:32] * left_on, value[32 : n - 32], value[n - 32 :] * right_on], axis=0
        )

    def spill_natural(value):
        n = value.shape[0]
        turned = [value] + [pltpu.roll(value, LANES - blk * j, axis=1) for j in range(1, 4)]
        del n
        return turned

    def windows_from_natural(value):
        n = value.shape[0]
        after = jnp.concatenate([value[8:], value[:8]], axis=0)
        mask = low_half(value.shape)
        put_window(0, n, jnp.where(mask, value, pltpu.roll(after, LANES // 2, axis=1)))
        put_window(
            1, n,
            jnp.where(mask, pltpu.roll(value, LANES - blk, axis=1), pltpu.roll(after, blk, axis=1)),
        )
        put_window(2, n, jnp.where(mask, pltpu.roll(value, LANES // 2, axis=1), after))

    def finish_pair(index):
        parts = block_ref[0, 0:cols, :], block_ref[1, 0:cols, :]
        both = quarters(parts[0], parts[0], parts[1], parts[1])
        out = own(both + smooth_own())
        basis_ref[index] = out
        return out

    def smooth_own():
        start = 32
        center = state_ref[1, start : start + cols, :]
        left = state_ref[1, start - 1 : start - 1 + cols, :]
        right = state_ref[1, start + 1 : start + 1 + cols, :]
        upper = pltpu.roll(center, 1, axis=1)
        lower = pltpu.roll(center, LANES - 1, axis=1)
        return PENALTY * (4.0 * center - upper - lower - left - right)

    def smooth_wide():
        n_out = total - 64
        start = 32
        center = state_ref[0, start : start + n_out, :]
        left = state_ref[0, start - 1 : start - 1 + n_out, :]
        right = state_ref[0, start + 1 : start + 1 + n_out, :]
        upper = pltpu.roll(center, 1, axis=1)
        lower = pltpu.roll(center, LANES - 1, axis=1)
        return PENALTY * (4.0 * center - upper - lower - left - right)

    loads[0].wait()
    build_tables()
    loads[1].wait()
    packed[0, 1, edge_g : edge_g + own_g] = pack(guess_ref[...])
    loads[2].wait()
    packed_right[0, 1, edge_g : edge_g + own_g] = pack(right_ref[...])
    pl.semaphore_wait(barrier, count - 1)
    send(packed, 0, 0)
    send(packed_right, 1, 0)

    n_mid = total - 64
    receive(packed, 0, 0)
    first_half(0)
    receive(packed_right, 1, 0)
    up_r, mid_r, down_r = (expand(packed_right[0, s]) for s in range(3))
    sl = slice(32, 32 + n_mid)
    nat_r = jnp.where(
        low_half((n_mid, LANES)),
        jnp.where(
            lax.broadcasted_iota(jnp.int32, (n_mid, LANES), 1) < blk,
            pltpu.roll(up_r[sl], LANES - blk, axis=1),
            pltpu.roll(mid_r[sl], blk, axis=1),
        ),
        jnp.where(
            lax.broadcasted_iota(jnp.int32, (n_mid, LANES), 1) < 3 * blk,
            pltpu.roll(mid_r[sl], blk, axis=1),
            pltpu.roll(down_r[sl], 3 * blk, axis=1),
        ),
    )
    start_residual = masked_natural(nat_r - (merge(n_mid) + smooth_wide()))
    state_ref[1, 0:n_mid, :] = start_residual
    basis_ref[3] = own(state_ref[0, edge : edge + cols, :])
    r0 = own(start_residual[32 : 32 + cols])
    basis_ref[0] = r0
    windows_from_natural(start_residual)
    convolve(0, 3, n_mid)
    for k in range(3):
        put_block(k, -16 + blk * k, assemble(k, n_mid), 16)
    second_half_b()
    w1 = finish_pair(1)
    turned = pltpu.roll(w1, LANES - blk, axis=1).reshape(own_g, 2, 8, LANES)
    turned_up = pltpu.roll(w1, blk, axis=1).reshape(own_g, 2, 8, LANES)
    pk = jnp.where(low_half((own_g, 8, LANES)), turned[:, 0], turned_up[:, 1])
    packed[1, 1, edge_g : edge_g + own_g] = pk
    send(packed, 2, 1)
    finish(packed, 0, 0)
    finish(packed_right, 1, 0)
    m0, m1, m2 = row_sum(r0 * r0), row_sum(r0 * w1), row_sum(w1 * w1)

    receive(packed, 2, 1)
    first_half(1)
    second = masked_natural(merge(n_mid) + smooth_wide())
    state_ref[1, 0:n_mid, :] = second
    w2 = own(second[32 : 32 + cols])
    basis_ref[2] = w2
    m3, m4 = row_sum(basis_ref[1] * w2), row_sum(w2 * w2)
    windows_from_natural(second)
    convolve(0, 3, n_mid)
    for k in range(3):
        put_block(k, -16 + blk * k, assemble(k, n_mid), 16)
    k_rows = [block_ref[k, 16 : 16 + cols, :] for k in range(3)]
    joined = quarters(k_rows[0], k_rows[1], k_rows[2], k_rows[2])
    inside_k = jnp.logical_and(lane1 >= 16, lane1 < 16 + rows)
    joined = jnp.where(inside_k, joined, 0.0)
    smooth2 = smooth_own()
    m5 = row_sum(joined * joined) + row_sum(w2 * smooth2)

    def fold(x):
        for k in (64, 32, 16):
            x = x + pltpu.roll(x, k, axis=1)
        return x

    line = jnp.zeros((1, LANES), jnp.float32)
    for k, m in enumerate((m0, m1, m2, m3, m4, m5)):
        at_k = jnp.logical_and(lane1 >= 16 * k, lane1 < 16 * (k + 1))
        line = jnp.where(at_k, fold(m), line)
    red[me] = line

    def red_copy(place):
        return pltpu.make_async_remote_copy(
            src_ref=red.at[me], dst_ref=red.at[me], send_sem=red_send.at[0], recv_sem=red_recv.at[0],
            device_id=place, device_id_type=MESH,
        )

    all_red = pltpu.make_async_remote_copy(
        src_ref=red.at[pl.ds(0, count - 1)], dst_ref=red.at[pl.ds(0, count - 1)],
        send_sem=red_send.at[0], recv_sem=red_recv.at[0],
        device_id=(row, col), device_id_type=MESH,
    )
    others(lambda place: red_copy(place).start())
    finish(packed, 2, 1)
    second_half_b()
    w3 = finish_pair(4)

    all_red.wait_recv()
    sums = jnp.sum(red[...], axis=0)
    m = [
        jnp.sum(
            jnp.where(jnp.logical_and(lane1 >= 16 * k, lane1 < 16 * (k + 1)), sums, 0.0),
            axis=1, keepdims=True,
        )
        for k in range(MOMENTS)
    ]

    def times(p, q):
        return sum(
            p[i] * q[j] * m[i + j] for i in range(len(p)) for j in range(len(q))
        )

    rho, pi = [jnp.ones((1, 1), jnp.float32)], [jnp.ones((1, 1), jnp.float32)]
    step_sum = []
    norm = m[0]
    for it in range(3):
        shifted = [jnp.zeros((1, 1), jnp.float32)] + pi
        alpha = norm / times(pi, shifted)
        step_sum = [
            (step_sum[i] if i < len(step_sum) else 0.0) + alpha * pi[i] for i in range(len(pi))
        ]
        rho = [
            (rho[i] if i < len(rho) else 0.0) - alpha * shifted[i] for i in range(len(shifted))
        ]
        if it < 2:
            norm_next = times(rho, rho)
            beta = norm_next / norm
            pi = [rho[i] + (beta * pi[i] if i < len(pi) else 0.0) for i in range(len(rho))]
            norm = norm_next

    r0, w1, w2 = basis_ref[0], basis_ref[1], basis_ref[2]
    template = basis_ref[3] + step_sum[0] * r0 + step_sum[1] * w1 + step_sum[2] * w2
    residual = rho[0] * r0 + rho[1] * w1 + rho[2] * w2 + rho[3] * w3
    for ref, value in ((template_ref, template), (residual_ref, residual)):
        for k in range(0, cols, LANES):
            ref[:, k : k + LANES] = value[k : k + LANES].T[blk : blk + rows]
    all_red.wait_send()


def on_device(n_row, n_col, right_side, initial_guess, kernel):
    rows, cols = right_side.shape
    total = cols + 2 * rows
    count = n_row * n_col
    shape = jax.ShapeDtypeStruct((rows, cols), jnp.float32)
    f32, bf16 = jnp.float32, jnp.bfloat16
    copies = len(DIRECTIONS)
    return pl.pallas_call(
        functools.partial(body, n_row, n_col),
        out_shape=(shape, shape),
        in_specs=[pl.BlockSpec(memory_space=pl.ANY)] * 3,
        out_specs=[pl.BlockSpec(memory_space=pltpu.VMEM)] * 2,
        scratch_shapes=[
            pltpu.VMEM((rows, cols), f32),
            pltpu.VMEM((rows, cols), f32),
            pltpu.VMEM(kernel.shape, f32),
            pltpu.VMEM((2, 3, total // 16, 8, LANES), f32),
            pltpu.VMEM((1, 3, total // 16, 8, LANES), f32),
            pltpu.VMEM((2, LANES, LANES), f32),
            pltpu.VMEM((2, 2, 2 * LANES, 2 * LANES), bf16),
            pltpu.VMEM((5 * total + 16, LANES), bf16),
            pltpu.VMEM((5 * total + 16, LANES), bf16),
            pltpu.VMEM((5 * total + 16, LANES), f32),
            pltpu.VMEM((5 * total + 16, LANES), f32),
            pltpu.VMEM((total, LANES), f32),
            pltpu.VMEM((5, total + 8, LANES), f32),
            pltpu.VMEM((2, total, LANES), f32),
            pltpu.VMEM((5, cols, LANES), f32),
            pltpu.VMEM((count, 1, LANES), f32),
            pltpu.SemaphoreType.DMA((3,)),
            pltpu.SemaphoreType.DMA((3, copies)),
            pltpu.SemaphoreType.DMA((3, copies)),
            pltpu.SemaphoreType.DMA((1,)),
            pltpu.SemaphoreType.DMA((1,)),
        ],
        compiler_params=pltpu.CompilerParams(collective_id=0, has_side_effects=True),
    )(right_side, initial_guess, kernel)


def solution(mesh):
    placed = (P("row", "col"), P("row", "col"), P())
    return jax.shard_map(
        functools.partial(on_device, mesh.shape["row"], mesh.shape["col"]),
        mesh=mesh,
        in_specs=placed,
        out_specs=(P("row", "col"), P("row", "col")),
        check_vma=False,
    )
```

```python
import functools

import jax
import jax.numpy as jnp
from jax import lax
from jax.experimental import pallas as pl
from jax.experimental.pallas import tpu as pltpu
from jax.sharding import PartitionSpec as P

PENALTY = 0.05
LANES = 128
PIECE = 16
PIECES = 64
STEPS = (8, 15, 20)
SUMS = 9
MESH = pl.DeviceIdType.MESH
DIRECTIONS = ((-1, 0), (1, 0), (-1, -1), (-1, 1), (1, -1), (1, 1), (0, -1), (0, 1))


NEAR = tuple((a, b) for a in (-1, 0, 1) for b in (-1, 0, 1) if (a, b) != (0, 0))
GREET = NEAR + ((0, -4), (0, 4))


def square(r, c):
    return tuple((a, b) for a in (-r, 0, r) for b in (-c, 0, c) if (a, b) != (0, 0))


def greetings(n_row, n_col):
    places = [(r, c) for r in range(n_row) for c in range(n_col)]

    def reach(place, offsets):
        near = ((place[0] + a, place[1] + b) for a, b in offsets)
        return [p for p in near if 0 <= p[0] < n_row and 0 <= p[1] < n_col]

    def hear(known, offsets):
        if any(p not in known[d] for d in places for p in reach(d, offsets)):
            return None
        return {d: known[d].union(*(known[p] for p in reach(d, offsets))) for d in places}

    known = {d: {d, *reach(d, GREET)} for d in places}
    known = hear(known, NEAR)
    rounds = []
    while min(map(len, known.values())) < len(places):
        best = None
        for r in range(1, max(2, n_row)):
            for c in range(1, max(2, n_col)):
                after = hear(known, square(r, c))
                if after is not None:
                    score = (min(map(len, after.values())), -r - c)
                    if best is None or score > best[0]:
                        best = (score, square(r, c), after)
        rounds.append(best[1])
        known = best[2]
    return rounds


def split(x):
    high = x.astype(jnp.bfloat16)
    low = (x - high.astype(jnp.float32)).astype(jnp.bfloat16)
    return high, low


def body(n_row, n_col, *refs):
    pieces = [
        pltpu.ACC(unit)((PIECE, 2 * LANES), jnp.float32) for unit in range(2) for _ in range(PIECES)
    ]

    def inner(*accs):
        run(n_row, n_col, (accs[:PIECES], accs[PIECES:]), *refs)

    pl.run_scoped(inner, *pieces)


def run(
    n_row, n_col, accs,
    right_hbm, guess_hbm, kernel_hbm, template_ref, residual_ref,
    right_ref, guess_ref, kernel_ref, first_pack, right_pack, second_pack,
    lines_ref, table, high_ref, low_ref, wide, partial_ref,
    state_ref, right_nat, own_ref, red, load_sem, send_sem, recv_sem, red_send, red_recv, known_sem,
):
    rows, cols = right_ref.shape
    row, col = lax.axis_index("row"), lax.axis_index("col")
    me, count = row * n_col + col, n_row * n_col
    width = kernel_ref.shape[0]
    blk = rows // 2
    own_g = cols // PIECE

    barrier = pltpu.get_barrier_semaphore()

    def within(dr, dc):
        return jnp.logical_and(
            jnp.logical_and(row + dr >= 0, row + dr < n_row),
            jnp.logical_and(col + dc >= 0, col + dc < n_col),
        )

    def greet(sem, offsets):
        for dr, dc in offsets:
            pl.when(within(dr, dc))(
                lambda dr=dr, dc=dc: pl.semaphore_signal(
                    sem, inc=1, device_id=(row + dr, col + dc), device_id_type=MESH
                )
            )

    def heard(offsets):
        return functools.reduce(jnp.add, [jnp.where(within(dr, dc), 1, 0) for dr, dc in offsets])

    greet(barrier, GREET)
    loads = [
        pltpu.make_async_copy(src, dst, load_sem.at[k])
        for k, (src, dst) in enumerate(
            ((guess_hbm, guess_ref), (right_hbm, right_ref), (kernel_hbm, kernel_ref))
        )
    ]
    for load in loads:
        load.start()

    lane1 = lax.broadcasted_iota(jnp.int32, (1, LANES), 1)

    def lanes_of(shape):
        return lax.broadcasted_iota(jnp.int32, shape, len(shape) - 1)

    def low_half(x):
        return lanes_of(x.shape) < LANES // 2

    def quarters(a, b, c, d):
        q = lanes_of(a.shape)
        return jnp.where(
            q < 2 * blk, jnp.where(q < blk, a, b), jnp.where(q < 3 * blk, c, d)
        )

    def turn(x, by):
        return pltpu.roll(x, by % LANES, axis=1)

    def inside(dr, dc):
        checks = []
        if dr:
            checks.append(row + dr >= 0 if dr < 0 else row + dr < n_row)
        if dc:
            checks.append(col + dc >= 0 if dc < 0 else col + dc < n_col)
        return functools.reduce(jnp.logical_and, checks)

    def clear(buf):
        groups = buf.shape[1]
        edge = (groups - own_g) // 2

        @pl.when(row == 0)
        def _():
            buf[0] = jnp.zeros(buf.shape[1:], jnp.float32)

        @pl.when(row == n_row - 1)
        def _():
            buf[2] = jnp.zeros(buf.shape[1:], jnp.float32)

        @pl.when(col == 0)
        def _():
            buf[:, 0:edge] = jnp.zeros((3, edge, 8, LANES), jnp.float32)

        @pl.when(col == n_col - 1)
        def _():
            buf[:, groups - edge : groups] = jnp.zeros((3, edge, 8, LANES), jnp.float32)

    def each(buf, turn_no, act, sign):
        groups = buf.shape[1]
        edge = (groups - own_g) // 2

        def one(index):
            dr, dc = DIRECTIONS[index]
            c_src, c_dst, c_len = (
                (edge, groups - edge, edge) if dc < 0
                else (own_g, 0, edge) if dc > 0
                else (edge, edge, own_g)
            )
            act(pltpu.make_async_remote_copy(
                src_ref=buf.at[1, pl.ds(c_src, c_len)],
                dst_ref=buf.at[1 - dr, pl.ds(c_dst, c_len)],
                send_sem=send_sem.at[turn_no, index],
                recv_sem=recv_sem.at[turn_no, index],
                device_id=(row + dr, col + dc),
                device_id_type=MESH,
            ))

        for index, (dr, dc) in enumerate(DIRECTIONS):
            pl.when(inside(sign * dr, sign * dc))(functools.partial(one, index))

    def send(buf, turn_no):
        each(buf, turn_no, lambda c: c.start(), 1)

    def receive(buf, turn_no):
        each(buf, turn_no, lambda c: c.wait_recv(), -1)

    def finish(buf, turn_no):
        each(buf, turn_no, lambda c: c.wait_send(), 1)

    def flip(x):
        return jnp.concatenate([x[a : a + 1] for a in reversed(range(width))] + [x[width:]], axis=0)

    def build_tables():
        taps = kernel_ref[...]
        taps = jnp.concatenate([taps, jnp.zeros((width, LANES - width), jnp.float32)], axis=1)
        taps = jnp.concatenate([taps, jnp.zeros((LANES - width, LANES), jnp.float32)], axis=0)
        lines_ref[0] = turn(flip(taps).T, -width)
        lines_ref[1] = turn(taps.T, -width)

        for which in range(2):
            for q in range(2):
                for h in range(2):
                    for half in range(2):
                        lines = []
                        for g in range(4):
                            b = 16 * q + 8 * h + 4 * half + g
                            source = b - 1 if which == 0 else width - b
                            if b == 0:
                                lines.append(jnp.zeros((8, LANES), jnp.float32))
                            else:
                                lines.append(
                                    jnp.broadcast_to(lines_ref[which, source : source + 1, :], (8, LANES))
                                )
                        tiles = []
                        for k in range(2 * blk // 8):
                            tiles.append(quarters(*(
                                pltpu.roll(
                                    lines[g], (blk * g + 8 * k) % LANES, axis=1, stride=1, stride_axis=0
                                )
                                for g in range(4)
                            )))
                        high, low = split(jnp.concatenate(tiles, axis=0))
                        at_row = pl.ds(LANES * q + 2 * blk * h, 2 * blk)
                        at_lane = pl.ds(LANES * half, LANES)
                        table[which, 0, at_row, at_lane] = high
                        table[which, 1, at_row, at_lane] = low

    def pack(tile):
        tall = jnp.concatenate([tile, pltpu.roll(tile, cols - 8, axis=1)], axis=0)
        pieces = [tall[:, k : k + LANES].T for k in range(0, cols, LANES)]
        form = jnp.concatenate(pieces, axis=0)
        return form.reshape(own_g, 2, 8, LANES)[:, 0]

    def expand(buf, tile, first, size):
        last = min(first + size, buf.shape[1] - 1)
        pk = buf[tile, first : first + size]
        after = buf[tile, last : last + 1]
        if size > 1:
            after = jnp.concatenate([pk[1:], after], axis=0)
        odd = jnp.where(low_half(pk), after, pk).reshape(-1, LANES)
        odd = turn(odd, LANES // 2).reshape(pk.shape)
        return jnp.stack([pk, odd], axis=1).reshape(size * 16, LANES)

    first_row, last_row = row == 0, row == n_row - 1
    left_on = jnp.where(col == 0, 0.0, 1.0)
    right_on = jnp.where(col == n_col - 1, 0.0, 1.0)

    def row_mask(at):
        off = jnp.logical_or(
            jnp.logical_and(at < 0, first_row), jnp.logical_and(at >= rows, last_row)
        )
        return jnp.where(off, 0.0, 1.0)

    def masked(value, start, margin, mask):
        out = []
        for j in range(start, start + value.shape[0], PIECE):
            piece = value[j - start : j - start + PIECE]
            side = mask
            if j < margin:
                side = mask * left_on
            elif j >= margin + cols:
                side = mask * right_on
            out.append(piece * side)
        return jnp.concatenate(out, axis=0) if len(out) > 1 else out[0]

    counters = {"piece": [0, 0], "stage": 0}

    def take(unit):
        acc = accs[unit][counters["piece"][unit] % PIECES]
        counters["piece"][unit] += 1
        return acc

    def put_window(slot, k, at, value):
        high, low = split(value)
        high_ref[slot, k, at : at + value.shape[0], :] = high
        low_ref[slot, k, at : at + value.shape[0], :] = low

    class Stage:
        def __init__(self, which, n, n_in, lag, emit, feed=None, before=None):
            self.which, self.n, self.n_in, self.emit, self.feed = which, n, n_in, emit, feed
            self.before = before
            self.slot = counters["stage"] % 2
            counters["stage"] += 1
            self.units, self.n_out = (n_in - 16) // PIECE, n_in - 32
            self.ends = [e for e in (step - lag for step in STEPS) if 0 < e < self.units] + [self.units]
            self.starts = [0] + self.ends[:-1]
            self.done_t = self.done_o = 0

        def cost(self, i):
            return self.n * ((self.ends[i] - self.starts[i] + 1) // 2) * 24

        def matmul(self, i):
            c0, c1, slot, n = self.starts[i], self.ends[i], self.slot, self.n
            if i == 0 and self.before is not None:
                self.before()
            if self.feed is not None:
                self.feed(slot, c1 * PIECE + PIECE)
            middle = (c0 + c1 + (i + 1) % 2) // 2
            share = (range(c0, middle), range(middle, c1))
            held = [[(k, u, take(unit)) for k in range(n) for u in share[unit]] for unit in range(2)]
            for part in range(2):
                for unit in range(2):
                    if held[unit]:
                        pltpu.matmul_push_rhs(
                            table[self.which, part], staging_register=part, mxu_index=unit
                        )
            for source, load in ((high_ref, 0), (low_ref, None), (high_ref, 1)):
                for unit in range(2):
                    for j, (k, u, acc) in enumerate(held[unit]):
                        at = PIECE * u
                        lhs = jnp.concatenate(
                            [source[slot, k, at : at + 16, :], source[slot, k, at + 16 : at + 32, :]], axis=1
                        )
                        pltpu.matmul_acc_lhs(acc, lhs, load_staged_rhs=load if j == 0 else None)
            self.held = held

        def pop(self):
            slot = self.slot
            for unit in range(2):
                for k, u, acc in self.held[unit]:
                    out = pltpu.matmul_pop(acc)
                    at = PIECE * u
                    wide[slot, 0, k, at : at + PIECE, :] = out[:, 0:LANES]
                    wide[slot, 1, k, at : at + PIECE, :] = out[:, LANES:]

        def vector(self, i):
            slot = self.slot
            rows_done = self.ends[i] * PIECE
            t0, t1 = self.done_t, rows_done - 8
            for k in range(self.n):
                partial_ref[slot, k, t0:t1, :] = wide[slot, 0, k, t0:t1, :] + wide[slot, 1, k, t0 + 4 : t1 + 4, :]
            self.done_t = t1
            o1 = min(rows_done - 16, self.n_out)
            o = self.done_o
            while o < o1:
                e = min(o - o % 32 + 32, o1)
                self.emit(1 - slot, o, e, functools.partial(taken, slot, o, e))
                o = e
            self.done_o = o1

    def pipeline(stages):
        lag = 540
        next_mm = [0] * len(stages)
        done = [[] for _ in stages]
        clock, pending = 0, []
        while any(n < len(st.ends) for n, st in zip(next_mm, stages)):
            options = []
            for s, st in enumerate(stages):
                i = next_mm[s]
                if i == len(st.ends):
                    continue
                ready = 0
                if s:
                    need = st.ends[i] + 3 if i + 1 < len(st.ends) else stages[s - 1].units
                    before = [t for e, t in zip(stages[s - 1].ends, done[s - 1]) if e >= need]
                    if not before:
                        continue
                    ready = before[0]
                options.append((max(ready, clock), s))
            start, s = min(options)
            st, i = stages[s], next_mm[s]
            for item in [p for p in pending if p[0] <= start]:
                item[1].vector(item[2])
                pending.remove(item)
            st.matmul(i)
            st.pop()
            next_mm[s] += 1
            clock = start + st.cost(i)
            done[s].append(clock + lag)
            pending.append((clock + 200, st, i))
        for item in pending:
            item[1].vector(item[2])

    def taken(slot, o, e, k, shift):
        return partial_ref[slot, k, o + shift : e + shift, :]

    def fold4(t, *source):
        out = 0.0
        for s in range(4):
            out = out + turn(quarters(*(t(source[(p + s) % 4], p) for p in range(4))), s * blk)
        return out

    class Windows:
        def __init__(self, n):
            self.n, self.kept, self.at = n, None, 0

        def make(self, slot, parts):
            size = parts[0].shape[0] - 16
            if self.n == 2:
                for k in range(2):
                    a, b = parts[k], parts[k + 1]
                    win = quarters(a[0:size], b[0:size], a[8 : size + 8], b[8 : size + 8])
                    put_window(slot, k, self.at, win)
                self.at += size
                return
            value, t32, t64, t96, extra = parts

            def lo(x):
                return x[0:size]

            def hi(x):
                return x[8 : size + 8]

            for k in range(self.n):
                if k == 0:
                    win = jnp.where(low_half(lo(value)), lo(value), hi(t64))
                elif k == 1:
                    win = jnp.where(low_half(lo(value)), lo(t96), hi(t32))
                elif k == 2:
                    win = jnp.where(low_half(lo(value)), lo(t64), hi(value))
                else:
                    win = quarters(lo(t32), lo(extra), hi(t96), hi(extra))
                put_window(slot, k, self.at, win)
            self.at += size

        def add(self, slot, value, extra=None):
            if self.n == 2:
                parts = value
            else:
                parts = [value, turn(value, blk), turn(value, 2 * blk), turn(value, 3 * blk), extra]
            if self.kept is not None:
                parts = [
                    None if new is None else jnp.concatenate([old, new], axis=0)
                    for old, new in zip(self.kept, parts)
                ]
            if parts[0].shape[0] > 16:
                self.make(slot, parts)
            self.kept = [None if p is None else p[p.shape[0] - 16 :] for p in parts]

        def end(self, slot):
            parts = [None if p is None else jnp.concatenate([p, p], axis=0) for p in self.kept]
            self.make(slot, parts)

    def smooth(index, start, end):
        center = state_ref[index, start:end, :]
        left = state_ref[index, start - 1 : end - 1, :]
        right = state_ref[index, start + 1 : end + 1, :]
        return PENALTY * (4.0 * center - turn(center, 1) - turn(center, -1) - left - right)

    def repack(buf, group, value):
        n = value.shape[0] // 16
        down, up = (turn(value, by).reshape(n, 2, 8, LANES) for by in (-blk, blk))
        buf[1, group : group + n] = jnp.where(low_half(down[:, 0]), down[:, 0], up[:, 1])

    class Feed:
        def __init__(self, buf):
            self.buf, self.at = buf, 0

        def __call__(self, slot, upto):
            upto = min(upto, self.buf.shape[1] * 16)
            while self.at < upto:
                self.two(slot, self.at // 16, min(2, (upto - self.at) // 16))

        def two(self, slot, first, size):
            up, mid, down = (expand(self.buf, s, first, size) for s in range(3))
            at = self.at
            odd = lax.rem(lanes_of(mid.shape), 2 * blk) >= blk
            upper = jnp.where(odd, turn(mid, blk), turn(up, -blk))
            lower = jnp.where(odd, turn(down, blk), turn(mid, -blk))
            for k, w in enumerate((up, upper, mid, lower, down)):
                put_window(slot, k, at, w)
            state_ref[0, at : at + size * 16, :] = jnp.where(low_half(mid), upper, turn(lower, 2 * blk))
            self.at += size * 16

    def row_sum(x):
        return jnp.sum(x, axis=0, keepdims=True)

    def red_copy(turn_no, place):
        return pltpu.make_async_remote_copy(
            src_ref=red.at[turn_no, me], dst_ref=red.at[turn_no, me],
            send_sem=red_send.at[turn_no], recv_sem=red_recv.at[turn_no],
            device_id=place, device_id_type=MESH,
        )

    def all_red(turn_no):
        return pltpu.make_async_remote_copy(
            src_ref=red.at[turn_no, pl.ds(0, count - 1)], dst_ref=red.at[turn_no, pl.ds(0, count - 1)],
            send_sem=red_send.at[turn_no], recv_sem=red_recv.at[turn_no],
            device_id=(row, col), device_id_type=MESH,
        )

    def flipped(x, n, bits):
        if n & (n - 1):
            return lax.rem(x + bits, n)
        for k in range(n.bit_length() - 1):
            if bits >> k & 1:
                x = x + (1 - 2 * lax.rem(x // (1 << k), 2)) * (1 << k)
        return x

    def spread(turn_no, line):
        red[turn_no, me] = line
        for r in reversed(range(n_row)):
            for c in reversed(range(n_col)):
                if r or c:
                    red_copy(turn_no, (flipped(row, n_row, r), flipped(col, n_col, c))).start()

    def gather(turn_no, groups):
        all_red(turn_no).wait_recv()
        line = jnp.sum(red[turn_no], axis=0)
        return [
            jnp.sum(
                jnp.where(jnp.logical_and(lane1 >= a, lane1 < b), line, 0.0), axis=1, keepdims=True
            )
            for a, b in groups
        ]

    right_groups = right_pack.shape[1]
    first_row_at, last_row_at = row == 0, row == n_row - 1

    def blank(where):
        right_pack[where] = jnp.zeros_like(right_pack[where])

    def right_form(half, s):
        x = right_ref[half * blk : half * blk + blk, :]
        tall = jnp.concatenate(
            [x if p == s else pltpu.roll(x, cols - 8 * ((p - s) % 4), axis=1) for p in range(4)], axis=0
        )
        pieces = [tall[:, k : k + LANES].T for k in range(0, cols, LANES)]
        return jnp.concatenate(pieces, axis=0).reshape(right_groups - 2, 4, 8, LANES)[:, 0]

    def each_right(act, sign):
        def one(index):
            dr, dc = DIRECTIONS[index]
            src, dst = {-1: (4, 3), 1: (5, 0), 0: (1, 1)}[dr]
            c_src, c_dst, c_len = (
                (1, right_groups - 1, 1) if dc < 0
                else (right_groups - 2, 0, 1) if dc > 0
                else (1, 1, right_groups - 2)
            )
            planes = 1 if dr else 2
            act(pltpu.make_async_remote_copy(
                src_ref=right_pack.at[pl.ds(src, planes), pl.ds(c_src, c_len)],
                dst_ref=right_pack.at[pl.ds(dst, planes), pl.ds(c_dst, c_len)],
                send_sem=send_sem.at[1, index],
                recv_sem=recv_sem.at[1, index],
                device_id=(row + dr, col + dc),
                device_id_type=MESH,
            ))

        for index, (dr, dc) in enumerate(DIRECTIONS):
            pl.when(inside(sign * dr, sign * dc))(functools.partial(one, index))

    def right_natural():
        each_right(lambda c: c.wait_recv(), -1)
        planes = [right_pack[k] for k in range(4)]
        for t in range(4):
            value = quarters(*(planes[(p - t) % 4].reshape(-1, LANES) for p in range(4)))
            right_nat[:, t] = turn(value, -blk * t).reshape(right_groups, 8, LANES)

    clear(first_pack)
    for at_edge, where in (
        (first_row_at, (slice(0, 1), slice(None))), (last_row_at, (slice(3, 4), slice(None))),
        (col == 0, (slice(0, 4), slice(0, 1))),
        (col == n_col - 1, (slice(0, 4), slice(right_groups - 1, right_groups))),
    ):
        pl.when(at_edge)(functools.partial(blank, where))
    clear(second_pack)
    edge1 = (first_pack.shape[1] - own_g) // 2
    edge2 = (second_pack.shape[1] - own_g) // 2
    loads[0].wait()
    first_pack[1, edge1 : edge1 + own_g] = pack(guess_ref[...])
    pl.semaphore_wait(barrier, heard(GREET))
    send(first_pack, 0)
    loads[1].wait()
    for plane, half, s in ((4, 0, 3), (5, 1, 0), (1, 0, 1), (2, 1, 2)):
        right_pack[plane, 1 : right_groups - 1] = right_form(half, s)
    each_right(lambda c: c.start(), 1)
    loads[2].wait()
    build_tables()

    mask48, mask32 = (row_mask(lane1 - k) for k in (48, 32))
    mask_low = row_mask(rows + 16 + 0 * lane1)
    masks16 = [row_mask(blk * k - 16 + lax.rem(lane1, blk)) for k in range(3)]
    own32 = jnp.logical_and(lane1 >= 32, lane1 < 32 + rows)
    own16 = jnp.logical_and(lane1 >= 16, lane1 < 16 + rows)
    dots = [0.0] * SUMS
    first_sums = [0.0, 0.0]
    n_in = first_pack.shape[1] * 16

    def own_part(o, e, margin):
        a, b = max(o, margin), min(e, margin + cols)
        return slice(a - margin, b - margin), slice(a - o, b - o), a < b

    step = {}

    def late_wait():
        step["m0"], step["m1"] = gather(0, ((0, 64), (64, 128)))
        step["alpha0"] = step["m0"] / step["m1"]

    def three_stages(buf, second):
        wins_b, wins_c, wins_d = Windows(4), Windows(3), Windows(2)

        def emit_a(slot, o, e, t):
            value = masked(fold4(t, 0, 1, 2, 3), o, 48, mask48)
            wins_b.add(slot, value, masked(fold4(t, 4, 4, 4, 4), o, 48, mask_low))
            if second:
                to, of, some = own_part(o, e, 48)
                if some:
                    own_ref[5, to, :] = turn(value, -blk)[of]
            if e == n_in - 32:
                wins_b.end(slot)

        def emit_b(slot, o, e, t):
            value = fold4(t, 0, 1, 2, 3) + smooth(0, o + 32, e + 32)
            if not second:
                value = right_nat[o // 32, :, :, :].reshape(32, LANES) - value if e - o == 32 else (
                    right_nat[o // 32, o % 32 // 8 : (o % 32 + e - o) // 8].reshape(e - o, LANES) - value
                )
            value = masked(value, o, 32, mask32)
            state_ref[1, o:e, :] = value
            wins_c.add(slot, value)
            if e == n_in - 64:
                wins_c.end(slot)
                if second:
                    products(step["alpha0"])

        def emit_c(slot, o, e, t):
            blocks = [masked(fold4(t, k, k, k, k), o, 16, masks16[k]) for k in range(3)]
            wins_d.add(slot, blocks)
            if second:
                to, of, some = own_part(o, e, 16)
                if some:
                    value = quarters(*(blocks[k][of] for k in (0, 1, 2, 2)))
                    value = jnp.where(own16, own_ref[5, to, :] - step["alpha0"] * value, 0.0)
                    dots[8] += row_sum(value * value)
            if e == n_in - 96:
                wins_d.end(slot)

        pipeline_of = [
            Stage(0, 5, n_in, 0, emit_a, Feed(buf)),
            Stage(1, 4, n_in - 32, 3, emit_b, before=late_wait if second else right_natural),
            Stage(0, 3, n_in - 64, 6, emit_c),
        ]
        return pipeline_of

    def products(alpha0):
        for o in range(0, cols, 32):
            e = o + 32
            r0 = own_ref[1, o:e, :]
            w1 = jnp.where(own32, state_ref[0, 64 + o : 64 + e, :], 0.0)
            w2 = jnp.where(own32, state_ref[1, 32 + o : 32 + e, :], 0.0)
            bend = smooth(0, 64 + o, 64 + e) - alpha0 * smooth(1, 32 + o, 32 + e)
            r1, q = r0 - alpha0 * w1, w1 - alpha0 * w2
            for k, x in ((2, w1), (3, w2), (4, q), (6, r1)):
                own_ref[k, o:e, :] = x
            for k, x in enumerate((r1 * r1, r1 * q, r1 * w1, w1 * w1, q * q, q * w1, q * w2, w1 * w2, q * bend)):
                dots[k] += row_sum(x)

    rounds = greetings(n_row, n_col)
    receive(first_pack, 0)
    if rounds:
        greet(known_sem.at[0], rounds[0])
    def emit_d(slot, o, e, t):
        r0 = jnp.where(own32, state_ref[1, o + 32 : e + 32, :], 0.0)
        w1 = jnp.where(own32, fold4(t, 0, 0, 1, 1) + smooth(1, o + 32, e + 32), 0.0)
        repack(second_pack, edge2 + o // 16, w1)
        own_ref[1, o:e, :] = r0
        own_ref[0, o:e, :] = state_ref[0, 64 + o : 64 + e, :]
        first_sums[0] += row_sum(r0 * r0)
        first_sums[1] += row_sum(r0 * w1)

    pipeline(three_stages(first_pack, False) + [Stage(1, 2, n_in - 96, 9, emit_d)])
    send(second_pack, 2)
    for k, offsets in enumerate(rounds):
        pl.semaphore_wait(known_sem.at[k], heard(offsets))
        if k + 1 < len(rounds):
            greet(known_sem.at[k + 1], rounds[k + 1])

    def fold(x, down_to):
        k = LANES // 2
        while k >= down_to:
            x = x + turn(x, k)
            k //= 2
        return x

    spread(0, jnp.where(lane1 < 64, fold(first_sums[0], 64), fold(first_sums[1], 64)))
    finish(first_pack, 0)
    each_right(lambda c: c.wait_send(), 1)

    receive(second_pack, 2)
    pipeline(three_stages(second_pack, True))
    m0, m1, alpha0 = step["m0"], step["m1"], step["alpha0"]
    line = fold(dots[8], 64)
    for k in range(8):
        line = jnp.where(jnp.logical_and(lane1 >= 8 * k, lane1 < 8 * k + 8), fold(dots[k], 8), line)
    spread(1, line)
    finish(second_pack, 2)
    all_red(0).wait_send()

    def emit_h(slot, o, e, t):
        w3 = jnp.where(own32, fold4(t, 0, 0, 1, 1) + smooth(1, o + 32, e + 32), 0.0)
        own_ref[5, o:e, :] = own_ref[3, o:e, :] - alpha0 * w3

    pipeline([Stage(1, 2, n_in - 96, 9, emit_h)])

    groups = [(8 * k, 8 * k + 8) for k in range(8)] + [(64, 128)]
    rr1, r1q, r1w, ww, qq, qw, qw2, ww2, qaq = gather(1, groups)
    beta0 = rr1 / m0
    alpha1 = rr1 / (r1q + beta0 * (2.0 * r1w + beta0 * m1))
    both = alpha1 * beta0
    rr2 = rr1 - 2.0 * alpha1 * (r1q + beta0 * r1w) + alpha1 * alpha1 * (
        qq + beta0 * (2.0 * qw + beta0 * ww)
    )
    beta1 = rr2 / rr1
    r2ar2 = (
        r1q + alpha1 * alpha1 * qaq + both * both * ww2
        - 2.0 * alpha1 * qq - 2.0 * both * qw + 2.0 * alpha1 * both * qw2
    )
    alpha2 = rr2 / (r2ar2 - beta1 * rr2 / alpha1)
    t_r0 = alpha0 + both + alpha2 * beta1 * beta0
    t_r1 = alpha1 + alpha2 * (1.0 + beta1)
    t_q, t_w1 = -alpha2 * alpha1, -alpha2 * both
    s_q, s_w1 = -alpha1 - alpha2 * (1.0 + beta1), -both - alpha2 * beta1 * beta0
    s_aq, s_w2 = alpha2 * alpha1, alpha2 * both
    for k in range(0, cols, LANES):
        r1, w1, w2, q, aq, r0 = (own_ref[i, k : k + LANES, :] for i in (6, 2, 3, 4, 5, 1))
        x0 = own_ref[0, k : k + LANES, :]
        template = x0 + t_r0 * r0 + t_r1 * r1 + t_q * q + t_w1 * w1
        residual = r1 + s_q * q + s_w1 * w1 + s_aq * aq + s_w2 * w2
        template_ref[:, k : k + LANES] = template.T[blk : blk + rows]
        residual_ref[:, k : k + LANES] = residual.T[blk : blk + rows]
    all_red(1).wait_send()


def on_device(n_row, n_col, right_side, initial_guess, kernel):
    rows, cols = right_side.shape
    count = n_row * n_col
    shape = pltpu.VMEM((rows, cols), jnp.float32)
    f32, bf16 = jnp.float32, jnp.bfloat16
    tall = cols + 2 * rows
    packs = [pltpu.VMEM((3, cols // 16 + 2 * (rows // 16), 8, LANES), f32) for _ in range(2)]
    packs.insert(1, pltpu.VMEM((6, cols // 32 + 2, 8, LANES), f32))
    return pl.pallas_call(
        functools.partial(body, n_row, n_col),
        out_shape=(shape, shape),
        in_specs=[pl.BlockSpec(memory_space=pl.ANY)] * 3,
        out_specs=[pl.BlockSpec(memory_space=pltpu.VMEM)] * 2,
        scratch_shapes=[
            pltpu.VMEM((rows, cols), f32),
            pltpu.VMEM((rows, cols), f32),
            pltpu.VMEM(kernel.shape, f32),
            *packs,
            pltpu.VMEM((2, LANES, LANES), f32),
            pltpu.VMEM((2, 2, 2 * LANES, 2 * LANES), bf16),
            pltpu.VMEM((2, 5, tall, LANES), bf16),
            pltpu.VMEM((2, 5, tall, LANES), bf16),
            pltpu.VMEM((2, 2, 5, tall, LANES), f32),
            pltpu.VMEM((2, 5, tall, LANES), f32),
            pltpu.VMEM((2, tall, LANES), f32),
            pltpu.VMEM((cols // 32 + 2, 4, 8, LANES), f32),
            pltpu.VMEM((7, cols, LANES), f32),
            pltpu.VMEM((2, count, 1, LANES), f32),
            pltpu.SemaphoreType.DMA((3,)),
            pltpu.SemaphoreType.DMA((3, len(DIRECTIONS))),
            pltpu.SemaphoreType.DMA((3, len(DIRECTIONS))),
            pltpu.SemaphoreType.DMA((2,)),
            pltpu.SemaphoreType.DMA((2,)),
            pltpu.SemaphoreType.REGULAR((len(greetings(n_row, n_col)),)),
        ],
        compiler_params=pltpu.CompilerParams(collective_id=0, has_side_effects=True),
    )(right_side, initial_guess, kernel)


def solution(mesh):
    placed = (P("row", "col"), P("row", "col"), P())
    return jax.shard_map(
        functools.partial(on_device, mesh.shape["row"], mesh.shape["col"]),
        mesh=mesh,
        in_specs=placed,
        out_specs=(P("row", "col"), P("row", "col")),
        check_vma=False,
    )
```

```python
import functools

import jax
import jax.numpy as jnp
from jax import lax
from jax.experimental import pallas as pl
from jax.experimental.pallas import tpu as pltpu
from jax.sharding import PartitionSpec as P

PENALTY = 0.05
LANES = 128
PIECE = 16
PIECES = 64
STEPS = (8, 15, 20)
SUMS = 9
MESH = pl.DeviceIdType.MESH
DIRECTIONS = ((-1, 0), (1, 0), (-1, -1), (-1, 1), (1, -1), (1, 1), (0, -1), (0, 1))


NEAR = tuple((a, b) for a in (-1, 0, 1) for b in (-1, 0, 1) if (a, b) != (0, 0))
GREET = NEAR + ((0, -4), (0, 4))


def square(r, c):
    return tuple((a, b) for a in (-r, 0, r) for b in (-c, 0, c) if (a, b) != (0, 0))


def greetings(n_row, n_col):
    places = [(r, c) for r in range(n_row) for c in range(n_col)]

    def reach(place, offsets):
        near = ((place[0] + a, place[1] + b) for a, b in offsets)
        return [p for p in near if 0 <= p[0] < n_row and 0 <= p[1] < n_col]

    def hear(known, offsets):
        if any(p not in known[d] for d in places for p in reach(d, offsets)):
            return None
        return {d: known[d].union(*(known[p] for p in reach(d, offsets))) for d in places}

    known = {d: {d, *reach(d, GREET)} for d in places}
    known = hear(known, NEAR)
    rounds = []
    while min(map(len, known.values())) < len(places):
        best = None
        for r in range(1, max(2, n_row)):
            for c in range(1, max(2, n_col)):
                after = hear(known, square(r, c))
                if after is not None:
                    score = (min(map(len, after.values())), -r - c)
                    if best is None or score > best[0]:
                        best = (score, square(r, c), after)
        rounds.append(best[1])
        known = best[2]
    return rounds


def split(x):
    high = x.astype(jnp.bfloat16)
    low = (x - high.astype(jnp.float32)).astype(jnp.bfloat16)
    return high, low


def body(n_row, n_col, *refs):
    pieces = [
        pltpu.ACC(unit)((PIECE, 2 * LANES), jnp.float32) for unit in range(2) for _ in range(PIECES)
    ]

    def inner(*accs):
        run(n_row, n_col, (accs[:PIECES], accs[PIECES:]), *refs)

    pl.run_scoped(inner, *pieces)


def run(
    n_row, n_col, accs,
    right_hbm, guess_hbm, kernel_hbm, template_ref, residual_ref, shared_ref,
    right_ref, guess_ref, kernel_ref, first_pack, right_pack, second_pack,
    lines_ref, table, high_ref, low_ref, wide, partial_ref,
    state_ref, right_nat, own_ref, red, load_sem, send_sem, recv_sem, red_send, red_recv, known_sem,
):
    rows, cols = right_ref.shape
    row, col = lax.axis_index("row"), lax.axis_index("col")
    me, count = row * n_col + col, n_row * n_col
    width = kernel_ref.shape[0]
    blk = rows // 2
    own_g = cols // PIECE

    barrier = pltpu.get_barrier_semaphore()

    def within(dr, dc):
        return jnp.logical_and(
            jnp.logical_and(row + dr >= 0, row + dr < n_row),
            jnp.logical_and(col + dc >= 0, col + dc < n_col),
        )

    def greet(sem, offsets):
        for dr, dc in offsets:
            pl.when(within(dr, dc))(
                lambda dr=dr, dc=dc: pl.semaphore_signal(
                    sem, inc=1, device_id=(row + dr, col + dc), device_id_type=MESH
                )
            )

    def heard(offsets):
        return functools.reduce(jnp.add, [jnp.where(within(dr, dc), 1, 0) for dr, dc in offsets])

    greet(barrier, GREET)
    loads = [
        pltpu.make_async_copy(src, dst, load_sem.at[k])
        for k, (src, dst) in enumerate(
            ((guess_hbm, guess_ref), (right_hbm, right_ref), (kernel_hbm, kernel_ref))
        )
    ]
    for load in loads:
        load.start()

    lane1 = lax.broadcasted_iota(jnp.int32, (1, LANES), 1)

    def lanes_of(shape):
        return lax.broadcasted_iota(jnp.int32, shape, len(shape) - 1)

    def low_half(x):
        return lanes_of(x.shape) < LANES // 2

    def quarters(a, b, c, d):
        q = lanes_of(a.shape)
        return jnp.where(
            q < 2 * blk, jnp.where(q < blk, a, b), jnp.where(q < 3 * blk, c, d)
        )

    def turn(x, by):
        return pltpu.roll(x, by % LANES, axis=1)

    def inside(dr, dc):
        checks = []
        if dr:
            checks.append(row + dr >= 0 if dr < 0 else row + dr < n_row)
        if dc:
            checks.append(col + dc >= 0 if dc < 0 else col + dc < n_col)
        return functools.reduce(jnp.logical_and, checks)

    def clear(buf):
        groups = buf.shape[1]
        edge = (groups - own_g) // 2

        @pl.when(row == 0)
        def _():
            buf[0] = jnp.zeros(buf.shape[1:], jnp.float32)

        @pl.when(row == n_row - 1)
        def _():
            buf[2] = jnp.zeros(buf.shape[1:], jnp.float32)

        @pl.when(col == 0)
        def _():
            buf[:, 0:edge] = jnp.zeros((3, edge, 8, LANES), jnp.float32)

        @pl.when(col == n_col - 1)
        def _():
            buf[:, groups - edge : groups] = jnp.zeros((3, edge, 8, LANES), jnp.float32)

    def each(buf, turn_no, act, sign):
        groups = buf.shape[1]
        edge = (groups - own_g) // 2

        def one(index):
            dr, dc = DIRECTIONS[index]
            c_src, c_dst, c_len = (
                (edge, groups - edge, edge) if dc < 0
                else (own_g, 0, edge) if dc > 0
                else (edge, edge, own_g)
            )
            act(pltpu.make_async_remote_copy(
                src_ref=buf.at[1, pl.ds(c_src, c_len)],
                dst_ref=buf.at[1 - dr, pl.ds(c_dst, c_len)],
                send_sem=send_sem.at[turn_no, index],
                recv_sem=recv_sem.at[turn_no, index],
                device_id=(row + dr, col + dc),
                device_id_type=MESH,
            ))

        for index, (dr, dc) in enumerate(DIRECTIONS):
            pl.when(inside(sign * dr, sign * dc))(functools.partial(one, index))

    def send(buf, turn_no):
        each(buf, turn_no, lambda c: c.start(), 1)

    def receive(buf, turn_no):
        each(buf, turn_no, lambda c: c.wait_recv(), -1)

    def finish(buf, turn_no):
        each(buf, turn_no, lambda c: c.wait_send(), 1)

    def flip(x):
        return jnp.concatenate([x[a : a + 1] for a in reversed(range(width))] + [x[width:]], axis=0)

    def build_tables():
        taps = kernel_ref[...]
        taps = jnp.concatenate([taps, jnp.zeros((width, LANES - width), jnp.float32)], axis=1)
        taps = jnp.concatenate([taps, jnp.zeros((LANES - width, LANES), jnp.float32)], axis=0)
        lines_ref[0] = turn(flip(taps).T, -width)
        lines_ref[1] = turn(taps.T, -width)

        for which in range(2):
            for q in range(2):
                for h in range(2):
                    for half in range(2):
                        lines = []
                        for g in range(4):
                            b = 16 * q + 8 * h + 4 * half + g
                            source = b - 1 if which == 0 else width - b
                            if b == 0:
                                lines.append(jnp.zeros((8, LANES), jnp.float32))
                            else:
                                lines.append(
                                    jnp.broadcast_to(lines_ref[which, source : source + 1, :], (8, LANES))
                                )
                        tiles = []
                        for k in range(2 * blk // 8):
                            tiles.append(quarters(*(
                                pltpu.roll(
                                    lines[g], (blk * g + 8 * k) % LANES, axis=1, stride=1, stride_axis=0
                                )
                                for g in range(4)
                            )))
                        high, low = split(jnp.concatenate(tiles, axis=0))
                        at_row = pl.ds(LANES * q + 2 * blk * h, 2 * blk)
                        at_lane = pl.ds(LANES * half, LANES)
                        table[which, 0, at_row, at_lane] = high
                        table[which, 1, at_row, at_lane] = low

    def pack(tile):
        tall = jnp.concatenate([tile, pltpu.roll(tile, cols - 8, axis=1)], axis=0)
        pieces = [tall[:, k : k + LANES].T for k in range(0, cols, LANES)]
        form = jnp.concatenate(pieces, axis=0)
        return form.reshape(own_g, 2, 8, LANES)[:, 0]

    def expand(buf, tile, first, size):
        last = min(first + size, buf.shape[1] - 1)
        pk = buf[tile, first : first + size]
        after = buf[tile, last : last + 1]
        if size > 1:
            after = jnp.concatenate([pk[1:], after], axis=0)
        odd = jnp.where(low_half(pk), after, pk).reshape(-1, LANES)
        odd = turn(odd, LANES // 2).reshape(pk.shape)
        return jnp.stack([pk, odd], axis=1).reshape(size * 16, LANES)

    first_row, last_row = row == 0, row == n_row - 1
    left_on = jnp.where(col == 0, 0.0, 1.0)
    right_on = jnp.where(col == n_col - 1, 0.0, 1.0)

    def row_mask(at):
        off = jnp.logical_or(
            jnp.logical_and(at < 0, first_row), jnp.logical_and(at >= rows, last_row)
        )
        return jnp.where(off, 0.0, 1.0)

    def masked(value, start, margin, mask):
        out = []
        for j in range(start, start + value.shape[0], PIECE):
            piece = value[j - start : j - start + PIECE]
            side = mask
            if j < margin:
                side = mask * left_on
            elif j >= margin + cols:
                side = mask * right_on
            out.append(piece * side)
        return jnp.concatenate(out, axis=0) if len(out) > 1 else out[0]

    counters = {"piece": [0, 0], "stage": 0}

    def take(unit):
        acc = accs[unit][counters["piece"][unit] % PIECES]
        counters["piece"][unit] += 1
        return acc

    def put_window(slot, k, at, value):
        high, low = split(value)
        high_ref[slot, k, at : at + value.shape[0], :] = high
        low_ref[slot, k, at : at + value.shape[0], :] = low

    class Stage:
        def __init__(self, which, n, n_in, lag, emit, feed=None, before=None):
            self.which, self.n, self.n_in, self.emit, self.feed = which, n, n_in, emit, feed
            self.before = before
            self.slot = counters["stage"] % 2
            counters["stage"] += 1
            self.units, self.n_out = (n_in - 16) // PIECE, n_in - 32
            self.ends = [e for e in (step - lag for step in STEPS) if 0 < e < self.units] + [self.units]
            self.starts = [0] + self.ends[:-1]
            self.done_t = self.done_o = 0

        def cost(self, i):
            return self.n * ((self.ends[i] - self.starts[i] + 1) // 2) * 24

        def matmul(self, i):
            c0, c1, slot, n = self.starts[i], self.ends[i], self.slot, self.n
            if i == 0 and self.before is not None:
                self.before()
            if self.feed is not None:
                self.feed(slot, c1 * PIECE + PIECE)
            middle = (c0 + c1 + (i + 1) % 2) // 2
            share = (range(c0, middle), range(middle, c1))
            held = [[(k, u, take(unit)) for k in range(n) for u in share[unit]] for unit in range(2)]
            for part in range(2):
                for unit in range(2):
                    if held[unit]:
                        pltpu.matmul_push_rhs(
                            table[self.which, part], staging_register=part, mxu_index=unit
                        )
            for source, load in ((high_ref, 0), (low_ref, None), (high_ref, 1)):
                for unit in range(2):
                    for j, (k, u, acc) in enumerate(held[unit]):
                        at = PIECE * u
                        lhs = jnp.concatenate(
                            [source[slot, k, at : at + 16, :], source[slot, k, at + 16 : at + 32, :]], axis=1
                        )
                        pltpu.matmul_acc_lhs(acc, lhs, load_staged_rhs=load if j == 0 else None)
            self.held = held

        def pop(self):
            slot = self.slot
            for unit in range(2):
                for k, u, acc in self.held[unit]:
                    out = pltpu.matmul_pop(acc)
                    at = PIECE * u
                    wide[slot, 0, k, at : at + PIECE, :] = out[:, 0:LANES]
                    wide[slot, 1, k, at : at + PIECE, :] = out[:, LANES:]

        def vector(self, i):
            slot = self.slot
            rows_done = self.ends[i] * PIECE
            t0, t1 = self.done_t, rows_done - 8
            for k in range(self.n):
                partial_ref[slot, k, t0:t1, :] = wide[slot, 0, k, t0:t1, :] + wide[slot, 1, k, t0 + 4 : t1 + 4, :]
            self.done_t = t1
            o1 = min(rows_done - 16, self.n_out)
            o = self.done_o
            while o < o1:
                e = min(o - o % 32 + 32, o1)
                self.emit(1 - slot, o, e, functools.partial(taken, slot, o, e))
                o = e
            self.done_o = o1

    def pipeline(stages):
        lag = 540
        next_mm = [0] * len(stages)
        done = [[] for _ in stages]
        clock, pending = 0, []
        while any(n < len(st.ends) for n, st in zip(next_mm, stages)):
            options = []
            for s, st in enumerate(stages):
                i = next_mm[s]
                if i == len(st.ends):
                    continue
                ready = 0
                if s:
                    need = st.ends[i] + 3 if i + 1 < len(st.ends) else stages[s - 1].units
                    before = [t for e, t in zip(stages[s - 1].ends, done[s - 1]) if e >= need]
                    if not before:
                        continue
                    ready = before[0]
                options.append((max(ready, clock), s))
            start, s = min(options)
            st, i = stages[s], next_mm[s]
            for item in [p for p in pending if p[0] <= start]:
                item[1].vector(item[2])
                pending.remove(item)
            st.matmul(i)
            st.pop()
            next_mm[s] += 1
            clock = start + st.cost(i)
            done[s].append(clock + lag)
            pending.append((clock + 200, st, i))
        for item in pending:
            item[1].vector(item[2])

    def taken(slot, o, e, k, shift):
        return partial_ref[slot, k, o + shift : e + shift, :]

    def fold4(t, *source):
        out = 0.0
        for s in range(4):
            out = out + turn(quarters(*(t(source[(p + s) % 4], p) for p in range(4))), s * blk)
        return out

    class Windows:
        def __init__(self, n, blocks=False):
            self.n, self.blocks, self.kept, self.at = n, blocks, None, 0

        def make(self, slot, parts):
            size = parts[0].shape[0] - 16
            if self.blocks:
                for k in range(self.n):
                    a, b = parts[k], parts[k + 1]
                    win = quarters(a[0:size], b[0:size], a[8 : size + 8], b[8 : size + 8])
                    put_window(slot, k, self.at, win)
                self.at += size
                return
            value, t32, t64, t96, extra = parts

            def lo(x):
                return x[0:size]

            def hi(x):
                return x[8 : size + 8]

            for k in range(self.n):
                if k == 0:
                    win = jnp.where(low_half(lo(value)), lo(value), hi(t64))
                elif k == 1:
                    win = jnp.where(low_half(lo(value)), lo(t96), hi(t32))
                elif k == 2:
                    win = jnp.where(low_half(lo(value)), lo(t64), hi(value))
                else:
                    win = quarters(lo(t32), lo(extra), hi(t96), hi(extra))
                put_window(slot, k, self.at, win)
            self.at += size

        def add(self, slot, value, extra=None):
            if self.blocks:
                parts = value
            else:
                parts = [value, turn(value, blk), turn(value, 2 * blk), turn(value, 3 * blk), extra]
            if self.kept is not None:
                parts = [
                    None if new is None else jnp.concatenate([old, new], axis=0)
                    for old, new in zip(self.kept, parts)
                ]
            if parts[0].shape[0] > 16:
                self.make(slot, parts)
            self.kept = [None if p is None else p[p.shape[0] - 16 :] for p in parts]

        def end(self, slot):
            parts = [None if p is None else jnp.concatenate([p, p], axis=0) for p in self.kept]
            self.make(slot, parts)

    def smooth(index, start, end):
        center = state_ref[index, start:end, :]
        left = state_ref[index, start - 1 : end - 1, :]
        right = state_ref[index, start + 1 : end + 1, :]
        return PENALTY * (4.0 * center - turn(center, 1) - turn(center, -1) - left - right)

    def repack(buf, group, value):
        n = value.shape[0] // 16
        down, up = (turn(value, by).reshape(n, 2, 8, LANES) for by in (-16, 48))
        q = lanes_of((n, 8, LANES))
        lower = jnp.where(q < 16, up[:, 0], down[:, 0])
        upper = jnp.where(q < 80, down[:, 1], up[:, 1])
        buf[1, group : group + n] = jnp.where(q < 64, lower, upper)

    def swap(x):
        odd = lax.rem(lanes_of(x.shape) // blk, 2) == 1
        return jnp.where(odd, turn(x, blk), turn(x, -blk))

    class RolledFeed:
        def __init__(self, buf, first):
            self.buf, self.first, self.at = buf, first, 0

        def __call__(self, slot, upto):
            upto = min(upto, (self.buf.shape[1] - 2 * self.first) * 16)
            while self.at < upto:
                size = min(2, (upto - self.at) // 16)
                self.two(slot, self.first + self.at // 16, size)
                self.at += size * 16

        def two(self, slot, first, size):
            up, mid, down = (expand(self.buf, k, first, size) for k in range(3))
            at = self.at
            q = lax.rem(lanes_of(mid.shape), 2 * blk)
            second = jnp.where(q < 16, up, mid)
            fourth = jnp.where(q < 16, mid, down)
            start = swap(jnp.where(q < 16, up, jnp.where(q < blk, mid, up)))
            third = swap(jnp.where(jnp.logical_and(q >= 16, q < blk), down, mid))
            for k, w in enumerate((start, second, third, fourth)):
                put_window(slot, k, at, w)
            state_ref[0, at : at + size * 16, :] = jnp.where(
                low_half(mid), second, turn(fourth, 2 * blk)
            )

    class Feed:
        def __init__(self, buf, rolled):
            self.buf, self.rolled, self.at = buf, rolled, 0

        def __call__(self, slot, upto):
            upto = min(upto, self.buf.shape[1] * 16)
            while self.at < upto:
                self.two(slot, self.at // 16, min(2, (upto - self.at) // 16))

        def two(self, slot, first, size):
            up, mid, down = (expand(self.buf, s, first, size) for s in range(3))
            at = self.at
            if self.rolled:
                far = lax.rem(lanes_of(mid.shape), 2 * blk) >= 48
                up, mid, down = (jnp.where(far, turn(x, 48), turn(x, -16)) for x in (up, mid, down))
            odd = lax.rem(lanes_of(mid.shape), 2 * blk) >= blk
            upper = jnp.where(odd, turn(mid, blk), turn(up, -blk))
            lower = jnp.where(odd, turn(down, blk), turn(mid, -blk))
            for k, w in enumerate((up, upper, mid, lower, down)):
                put_window(slot, k, at, w)
            state_ref[0, at : at + size * 16, :] = jnp.where(low_half(mid), upper, turn(lower, 2 * blk))
            self.at += size * 16

    def row_sum(x):
        return jnp.sum(x, axis=0, keepdims=True)

    def red_copy(turn_no, place):
        return pltpu.make_async_remote_copy(
            src_ref=red.at[turn_no, me], dst_ref=red.at[turn_no, me],
            send_sem=red_send.at[turn_no], recv_sem=red_recv.at[turn_no],
            device_id=place, device_id_type=MESH,
        )

    def all_red(turn_no):
        return pltpu.make_async_remote_copy(
            src_ref=red.at[turn_no, pl.ds(0, count - 1)], dst_ref=red.at[turn_no, pl.ds(0, count - 1)],
            send_sem=red_send.at[turn_no], recv_sem=red_recv.at[turn_no],
            device_id=(row, col), device_id_type=MESH,
        )

    def flipped(x, n, bits):
        if n & (n - 1):
            return lax.rem(x + bits, n)
        for k in range(n.bit_length() - 1):
            if bits >> k & 1:
                x = x + (1 - 2 * lax.rem(x // (1 << k), 2)) * (1 << k)
        return x

    def spread(turn_no, line):
        red[turn_no, me] = line
        for r in reversed(range(n_row)):
            for c in reversed(range(n_col)):
                if r or c:
                    red_copy(turn_no, (flipped(row, n_row, r), flipped(col, n_col, c))).start()

    def gather(turn_no, groups):
        all_red(turn_no).wait_recv()
        line = jnp.sum(red[turn_no], axis=0)
        return [
            jnp.sum(
                jnp.where(jnp.logical_and(lane1 >= a, lane1 < b), line, 0.0), axis=1, keepdims=True
            )
            for a, b in groups
        ]

    right_groups = right_pack.shape[1]
    first_row_at, last_row_at = row == 0, row == n_row - 1

    def blank(where):
        right_pack[where] = jnp.zeros_like(right_pack[where])

    def right_form(half, s):
        x = right_ref[half * blk : half * blk + blk, :]
        tall = jnp.concatenate(
            [x if p == s else pltpu.roll(x, cols - 8 * ((p - s) % 4), axis=1) for p in range(4)], axis=0
        )
        pieces = [tall[:, k : k + LANES].T for k in range(0, cols, LANES)]
        return jnp.concatenate(pieces, axis=0).reshape(right_groups - 2, 4, 8, LANES)[:, 0]

    def each_right(act, sign):
        def one(index):
            dr, dc = DIRECTIONS[index]
            src, dst = {-1: (4, 3), 1: (5, 0), 0: (1, 1)}[dr]
            c_src, c_dst, c_len = (
                (1, right_groups - 1, 1) if dc < 0
                else (right_groups - 2, 0, 1) if dc > 0
                else (1, 1, right_groups - 2)
            )
            planes = 1 if dr else 2
            act(pltpu.make_async_remote_copy(
                src_ref=right_pack.at[pl.ds(src, planes), pl.ds(c_src, c_len)],
                dst_ref=right_pack.at[pl.ds(dst, planes), pl.ds(c_dst, c_len)],
                send_sem=send_sem.at[1, index],
                recv_sem=recv_sem.at[1, index],
                device_id=(row + dr, col + dc),
                device_id_type=MESH,
            ))

        for index, (dr, dc) in enumerate(DIRECTIONS):
            pl.when(inside(sign * dr, sign * dc))(functools.partial(one, index))

    def right_natural():
        each_right(lambda c: c.wait_recv(), -1)
        planes = [right_pack[k] for k in range(4)]
        for t in range(4):
            value = quarters(*(planes[(p - t) % 4].reshape(-1, LANES) for p in range(4)))
            right_nat[:, t] = turn(value, -blk * t).reshape(right_groups, 8, LANES)

    clear(first_pack)
    for at_edge, where in (
        (first_row_at, (slice(0, 1), slice(None))), (last_row_at, (slice(3, 4), slice(None))),
        (col == 0, (slice(0, 4), slice(0, 1))),
        (col == n_col - 1, (slice(0, 4), slice(right_groups - 1, right_groups))),
    ):
        pl.when(at_edge)(functools.partial(blank, where))
    clear(second_pack)
    edge1 = (first_pack.shape[1] - own_g) // 2
    edge2 = (second_pack.shape[1] - own_g) // 2
    loads[0].wait()
    first_pack[1, edge1 : edge1 + own_g] = pack(guess_ref[...])
    pl.semaphore_wait(barrier, heard(GREET))
    send(first_pack, 0)
    loads[1].wait()
    for plane, half, s in ((4, 0, 3), (5, 1, 0), (1, 0, 1), (2, 1, 2)):
        right_pack[plane, 1 : right_groups - 1] = right_form(half, s)
    each_right(lambda c: c.start(), 1)
    loads[2].wait()
    build_tables()

    mask48, mask32, mask16 = (row_mask(lane1 - k) for k in (48, 32, 16))
    mask_low = row_mask(rows + 16 + 0 * lane1)
    masks16 = [row_mask(blk * k - 16 + lax.rem(lane1, blk)) for k in range(3)]
    own32 = jnp.logical_and(lane1 >= 32, lane1 < 32 + rows)
    own16 = jnp.logical_and(lane1 >= 16, lane1 < 16 + rows)
    dots = [0.0] * SUMS
    first_sums = [0.0, 0.0]
    n_in = first_pack.shape[1] * 16

    def own_part(o, e, margin):
        a, b = max(o, margin), min(e, margin + cols)
        return slice(a - margin, b - margin), slice(a - o, b - o), a < b

    step = {}

    def late_wait():
        step["m0"], step["m1"] = gather(0, ((0, 64), (64, 128)))
        step["alpha0"] = step["m0"] / step["m1"]

    def three_stages(buf, second):
        wins_b, wins_c, wins_d = Windows(4), Windows(3), Windows(2, True)

        def emit_a(slot, o, e, t):
            value = masked(fold4(t, 0, 1, 2, 3), o, 48, mask48)
            wins_b.add(slot, value, masked(fold4(t, 4, 4, 4, 4), o, 48, mask_low))
            if e == n_in - 32:
                wins_b.end(slot)

        def emit_b(slot, o, e, t):
            value = fold4(t, 0, 1, 2, 3) + smooth(0, o + 32, e + 32)
            if not second:
                value = right_nat[o // 32, :, :, :].reshape(32, LANES) - value if e - o == 32 else (
                    right_nat[o // 32, o % 32 // 8 : (o % 32 + e - o) // 8].reshape(e - o, LANES) - value
                )
            value = masked(value, o, 32, mask32)
            state_ref[1, o:e, :] = value
            wins_c.add(slot, value)
            if e == n_in - 64:
                wins_c.end(slot)

        def emit_c(slot, o, e, t):
            blocks = [masked(fold4(t, k, k, k, k), o, 16, masks16[k]) for k in range(3)]
            wins_d.add(slot, blocks)
            if e == n_in - 96:
                wins_d.end(slot)

        pipeline_of = [
            Stage(0, 5, n_in, 0, emit_a, Feed(buf, second)),
            Stage(1, 4, n_in - 32, 3, emit_b, before=None if second else right_natural),
            Stage(0, 3, n_in - 64, 6, emit_c),
        ]
        return pipeline_of

    def early_stages(buf):
        wins_f, wins_g = Windows(3), Windows(2)
        n_two = n_in - 32

        def emit_e(slot, o, e, t):
            value = masked(fold4(t, 0, 1, 2, 3), o, 32, mask32)
            to, of, some = own_part(o, e, 32)
            if some:
                own_ref[5, to, :] = value[of]
            wins_f.add(slot, value)
            if e == n_two - 32:
                wins_f.end(slot)

        def emit_f(slot, o, e, t):
            value = masked(fold4(t, 0, 1, 2, 2) + smooth(0, o + 32, e + 32), o, 16, mask16)
            state_ref[1, o:e, :] = value
            wins_g.add(slot, value)
            if e == n_two - 64:
                wins_g.end(slot)
                products(step["alpha0"])

        def emit_g(slot, o, e, t):
            value = jnp.where(own32, own_ref[5, o:e, :] - step["alpha0"] * fold4(t, 0, 0, 1, 1), 0.0)
            dots[8] += row_sum(value * value)

        return [
            Stage(0, 4, n_two, 2, emit_e, RolledFeed(buf, 1)),
            Stage(1, 3, n_two - 32, 5, emit_f, before=late_wait),
            Stage(0, 2, n_two - 64, 8, emit_g),
        ]

    def products(alpha0):
        for o in range(0, cols, 32):
            e = o + 32
            r0 = own_ref[1, o:e, :]
            w1 = jnp.where(own16, state_ref[0, 48 + o : 48 + e, :], 0.0)
            w2 = jnp.where(own16, state_ref[1, 16 + o : 16 + e, :], 0.0)
            bend = smooth(0, 48 + o, 48 + e) - alpha0 * smooth(1, 16 + o, 16 + e)
            r1, q = r0 - alpha0 * w1, w1 - alpha0 * w2
            for k, x in ((2, w1), (3, w2), (4, q), (6, r1)):
                own_ref[k, o:e, :] = x
            for k, x in enumerate((r1 * r1, r1 * q, r1 * w1, w1 * w1, q * q, q * w1, q * w2, w1 * w2, q * bend)):
                dots[k] += row_sum(x)

    rounds = greetings(n_row, n_col)
    receive(first_pack, 0)
    if rounds:
        greet(known_sem.at[0], rounds[0])
    def emit_d(slot, o, e, t):
        r0 = jnp.where(own32, state_ref[1, o + 32 : e + 32, :], 0.0)
        w1 = jnp.where(own32, fold4(t, 0, 0, 1, 1) + smooth(1, o + 32, e + 32), 0.0)
        repack(second_pack, edge2 + o // 16, w1)
        first_sums[0] += row_sum(r0 * r0)
        first_sums[1] += row_sum(r0 * w1)

    pipeline(three_stages(first_pack, False) + [Stage(1, 2, n_in - 96, 9, emit_d)])
    send(second_pack, 2)
    for k, offsets in enumerate(rounds):
        pl.semaphore_wait(known_sem.at[k], heard(offsets))
        if k + 1 < len(rounds):
            greet(known_sem.at[k + 1], rounds[k + 1])

    def fold(x, down_to):
        k = LANES // 2
        while k >= down_to:
            x = x + turn(x, k)
            k //= 2
        return x

    spread(0, jnp.where(lane1 < 64, fold(first_sums[0], 64), fold(first_sums[1], 64)))
    finish(first_pack, 0)
    each_right(lambda c: c.wait_send(), 1)

    own_ref[0] = jnp.where(own16, turn(state_ref[0, 64 : 64 + cols, :], -16), 0.0)
    own_ref[1] = jnp.where(own16, turn(state_ref[1, 32 : 32 + cols, :], -16), 0.0)
    receive(second_pack, 2)
    pipeline(early_stages(second_pack))
    m0, m1, alpha0 = step["m0"], step["m1"], step["alpha0"]
    line = fold(dots[8], 64)
    for k in range(8):
        line = jnp.where(jnp.logical_and(lane1 >= 8 * k, lane1 < 8 * k + 8), fold(dots[k], 8), line)
    spread(1, line)
    finish(second_pack, 2)
    all_red(0).wait_send()

    def emit_h(slot, o, e, t):
        w3 = jnp.where(own32, fold4(t, 0, 0, 1, 1) + smooth(1, o + 32, e + 32), 0.0)
        w3 = turn(w3, -16)
        own_ref[5, o:e, :] = own_ref[3, o:e, :] - alpha0 * w3

    pipeline(three_stages(second_pack, True) + [Stage(1, 2, n_in - 96, 9, emit_h)])

    for k in range(0, cols, LANES):
        shared_ref[:, k : k + LANES] = own_ref[6, k : k + LANES, :].T[16 : 16 + rows]

    groups = [(8 * k, 8 * k + 8) for k in range(8)] + [(64, 128)]
    rr1, r1q, r1w, ww, qq, qw, qw2, ww2, qaq = gather(1, groups)
    beta0 = rr1 / m0
    alpha1 = rr1 / (r1q + beta0 * (2.0 * r1w + beta0 * m1))
    both = alpha1 * beta0
    rr2 = rr1 - 2.0 * alpha1 * (r1q + beta0 * r1w) + alpha1 * alpha1 * (
        qq + beta0 * (2.0 * qw + beta0 * ww)
    )
    beta1 = rr2 / rr1
    r2ar2 = (
        r1q + alpha1 * alpha1 * qaq + both * both * ww2
        - 2.0 * alpha1 * qq - 2.0 * both * qw + 2.0 * alpha1 * both * qw2
    )
    alpha2 = rr2 / (r2ar2 - beta1 * rr2 / alpha1)
    t_r0 = alpha0 + both + alpha2 * beta1 * beta0
    t_r1 = alpha1 + alpha2 * (1.0 + beta1)
    t_q, t_w1 = -alpha2 * alpha1, -alpha2 * both
    s_q, s_w1 = -alpha1 - alpha2 * (1.0 + beta1), -both - alpha2 * beta1 * beta0
    s_aq, s_w2 = alpha2 * alpha1, alpha2 * both
    for k in range(0, cols, LANES):
        r1, w1, w2, q, aq, r0 = (own_ref[i, k : k + LANES, :] for i in (6, 2, 3, 4, 5, 1))
        x0 = own_ref[0, k : k + LANES, :]
        template = x0 + t_r0 * r0 + (t_r1 - 1.0) * r1 + t_q * q + t_w1 * w1
        residual = s_q * q + s_w1 * w1 + s_aq * aq + s_w2 * w2
        template_ref[:, k : k + LANES] = template.T[16 : 16 + rows]
        residual_ref[:, k : k + LANES] = residual.T[16 : 16 + rows]
    all_red(1).wait_send()


def on_device(n_row, n_col, right_side, initial_guess, kernel):
    rows, cols = right_side.shape
    count = n_row * n_col
    shape = pltpu.VMEM((rows, cols), jnp.float32)
    f32, bf16 = jnp.float32, jnp.bfloat16
    tall = cols + 2 * rows
    packs = [pltpu.VMEM((3, cols // 16 + 2 * (rows // 16), 8, LANES), f32) for _ in range(2)]
    packs.insert(1, pltpu.VMEM((6, cols // 32 + 2, 8, LANES), f32))
    template, residual, shared = pl.pallas_call(
        functools.partial(body, n_row, n_col),
        out_shape=(shape,) * 3,
        in_specs=[pl.BlockSpec(memory_space=pl.ANY)] * 3,
        out_specs=[pl.BlockSpec(memory_space=pltpu.VMEM)] * 3,
        scratch_shapes=[
            pltpu.VMEM((rows, cols), f32),
            pltpu.VMEM((rows, cols), f32),
            pltpu.VMEM(kernel.shape, f32),
            *packs,
            pltpu.VMEM((2, LANES, LANES), f32),
            pltpu.VMEM((2, 2, 2 * LANES, 2 * LANES), bf16),
            pltpu.VMEM((2, 5, tall, LANES), bf16),
            pltpu.VMEM((2, 5, tall, LANES), bf16),
            pltpu.VMEM((2, 2, 5, tall, LANES), f32),
            pltpu.VMEM((2, 5, tall, LANES), f32),
            pltpu.VMEM((2, tall, LANES), f32),
            pltpu.VMEM((cols // 32 + 2, 4, 8, LANES), f32),
            pltpu.VMEM((7, cols, LANES), f32),
            pltpu.VMEM((2, count, 1, LANES), f32),
            pltpu.SemaphoreType.DMA((3,)),
            pltpu.SemaphoreType.DMA((3, len(DIRECTIONS))),
            pltpu.SemaphoreType.DMA((3, len(DIRECTIONS))),
            pltpu.SemaphoreType.DMA((2,)),
            pltpu.SemaphoreType.DMA((2,)),
            pltpu.SemaphoreType.REGULAR((len(greetings(n_row, n_col)),)),
        ],
        compiler_params=pltpu.CompilerParams(collective_id=0, has_side_effects=True),
    )(right_side, initial_guess, kernel)
    return template + shared, residual + shared


def solution(mesh):
    placed = (P("row", "col"), P("row", "col"), P())
    return jax.shard_map(
        functools.partial(on_device, mesh.shape["row"], mesh.shape["col"]),
        mesh=mesh,
        in_specs=placed,
        out_specs=(P("row", "col"), P("row", "col")),
        check_vma=False,
    )
```

```python
import functools

import jax
import jax.numpy as jnp
from jax import lax
from jax.experimental import pallas as pl
from jax.experimental.pallas import tpu as pltpu
from jax.sharding import PartitionSpec as P

PENALTY = 0.05
LANES = 128
PIECE = 16
PIECES = 64
STEPS = (8, 15, 20)
SUMS = 9
MESH = pl.DeviceIdType.MESH
DIRECTIONS = ((-1, -1), (-1, 1), (1, -1), (1, 1), (-1, 0), (1, 0), (0, -1), (0, 1))


NEAR = tuple((a, b) for a in (-1, 0, 1) for b in (-1, 0, 1) if (a, b) != (0, 0))
GREET = NEAR + ((0, -4), (0, 4))


def square(r, c):
    return tuple((a, b) for a in (-r, 0, r) for b in (-c, 0, c) if (a, b) != (0, 0))


def greetings(n_row, n_col):
    places = [(r, c) for r in range(n_row) for c in range(n_col)]

    def reach(place, offsets):
        near = ((place[0] + a, place[1] + b) for a, b in offsets)
        return [p for p in near if 0 <= p[0] < n_row and 0 <= p[1] < n_col]

    def hear(known, offsets):
        if any(p not in known[d] for d in places for p in reach(d, offsets)):
            return None
        return {d: known[d].union(*(known[p] for p in reach(d, offsets))) for d in places}

    known = {d: {d, *reach(d, GREET)} for d in places}
    known = hear(known, NEAR)
    rounds = []
    while min(map(len, known.values())) < len(places):
        best = None
        for r in range(1, max(2, n_row)):
            for c in range(1, max(2, n_col)):
                after = hear(known, square(r, c))
                if after is not None:
                    score = (min(map(len, after.values())), -r - c)
                    if best is None or score > best[0]:
                        best = (score, square(r, c), after)
        rounds.append(best[1])
        known = best[2]
    return rounds


def split(x):
    high = x.astype(jnp.bfloat16)
    low = (x - high.astype(jnp.float32)).astype(jnp.bfloat16)
    return high, low


def body(n_row, n_col, *refs):
    pieces = [
        pltpu.ACC(unit)((PIECE, 2 * LANES), jnp.float32) for unit in range(2) for _ in range(PIECES)
    ]

    def inner(*accs):
        run(n_row, n_col, (accs[:PIECES], accs[PIECES:]), *refs)

    pl.run_scoped(inner, *pieces)


def run(
    n_row, n_col, accs,
    right_hbm, guess_hbm, kernel_hbm, template_ref, residual_ref, shared_ref,
    right_ref, guess_ref, kernel_ref, first_pack, right_pack, second_pack,
    lines_ref, table, high_ref, low_ref, wide, partial_ref,
    state_ref, right_nat, own_ref, upright_ref, red, load_sem, send_sem, recv_sem, red_send, red_recv, known_sem,
):
    rows, cols = right_ref.shape
    row, col = lax.axis_index("row"), lax.axis_index("col")
    me, count = row * n_col + col, n_row * n_col
    width = kernel_ref.shape[0]
    blk = rows // 2
    own_g = cols // PIECE

    barrier = pltpu.get_barrier_semaphore()

    def within(dr, dc):
        return jnp.logical_and(
            jnp.logical_and(row + dr >= 0, row + dr < n_row),
            jnp.logical_and(col + dc >= 0, col + dc < n_col),
        )

    def greet(sem, offsets):
        for dr, dc in offsets:
            pl.when(within(dr, dc))(
                lambda dr=dr, dc=dc: pl.semaphore_signal(
                    sem, inc=1, device_id=(row + dr, col + dc), device_id_type=MESH
                )
            )

    def heard(offsets):
        return functools.reduce(jnp.add, [jnp.where(within(dr, dc), 1, 0) for dr, dc in offsets])

    greet(barrier, GREET)
    loads = [
        pltpu.make_async_copy(src, dst, load_sem.at[k])
        for k, (src, dst) in enumerate(
            ((guess_hbm, guess_ref), (right_hbm, right_ref), (kernel_hbm, kernel_ref))
        )
    ]
    for load in loads:
        load.start()

    lane1 = lax.broadcasted_iota(jnp.int32, (1, LANES), 1)

    def lanes_of(shape):
        return lax.broadcasted_iota(jnp.int32, shape, len(shape) - 1)

    def low_half(x):
        return lanes_of(x.shape) < LANES // 2

    def quarters(a, b, c, d):
        q = lanes_of(a.shape)
        return jnp.where(
            q < 2 * blk, jnp.where(q < blk, a, b), jnp.where(q < 3 * blk, c, d)
        )

    def turn(x, by):
        return pltpu.roll(x, by % LANES, axis=1)

    def inside(dr, dc):
        checks = []
        if dr:
            checks.append(row + dr >= 0 if dr < 0 else row + dr < n_row)
        if dc:
            checks.append(col + dc >= 0 if dc < 0 else col + dc < n_col)
        return functools.reduce(jnp.logical_and, checks)

    def clear(buf):
        groups = buf.shape[1]
        edge = (groups - own_g) // 2

        @pl.when(row == 0)
        def _():
            buf[0] = jnp.zeros(buf.shape[1:], jnp.float32)

        @pl.when(row == n_row - 1)
        def _():
            buf[2] = jnp.zeros(buf.shape[1:], jnp.float32)

        @pl.when(col == 0)
        def _():
            buf[:, 0:edge] = jnp.zeros((3, edge, 8, LANES), jnp.float32)

        @pl.when(col == n_col - 1)
        def _():
            buf[:, groups - edge : groups] = jnp.zeros((3, edge, 8, LANES), jnp.float32)

    def each(buf, turn_no, act, sign):
        groups = buf.shape[1]
        edge = (groups - own_g) // 2

        def one(index):
            dr, dc = DIRECTIONS[index]
            c_src, c_dst, c_len = (
                (edge, groups - edge, edge) if dc < 0
                else (own_g, 0, edge) if dc > 0
                else (edge, edge, own_g)
            )
            act(pltpu.make_async_remote_copy(
                src_ref=buf.at[1, pl.ds(c_src, c_len)],
                dst_ref=buf.at[1 - dr, pl.ds(c_dst, c_len)],
                send_sem=send_sem.at[turn_no, index],
                recv_sem=recv_sem.at[turn_no, index],
                device_id=(row + dr, col + dc),
                device_id_type=MESH,
            ))

        for index, (dr, dc) in enumerate(DIRECTIONS):
            pl.when(inside(sign * dr, sign * dc))(functools.partial(one, index))

    def send(buf, turn_no):
        each(buf, turn_no, lambda c: c.start(), 1)

    def receive(buf, turn_no):
        each(buf, turn_no, lambda c: c.wait_recv(), -1)

    def finish(buf, turn_no):
        each(buf, turn_no, lambda c: c.wait_send(), 1)

    def flip(x):
        return jnp.concatenate([x[a : a + 1] for a in reversed(range(width))] + [x[width:]], axis=0)

    def build_tables():
        taps = kernel_ref[...]
        taps = jnp.concatenate([taps, jnp.zeros((width, LANES - width), jnp.float32)], axis=1)
        taps = jnp.concatenate([taps, jnp.zeros((LANES - width, LANES), jnp.float32)], axis=0)
        lines_ref[0] = turn(flip(taps).T, -width)
        lines_ref[1] = turn(taps.T, -width)

        for which in range(2):
            for q in range(2):
                for h in range(2):
                    for half in range(2):
                        lines = []
                        for g in range(4):
                            b = 16 * q + 8 * h + 4 * half + g
                            source = b - 1 if which == 0 else width - b
                            if b == 0:
                                lines.append(jnp.zeros((8, LANES), jnp.float32))
                            else:
                                lines.append(
                                    jnp.broadcast_to(lines_ref[which, source : source + 1, :], (8, LANES))
                                )
                        tiles = []
                        for k in range(2 * blk // 8):
                            tiles.append(quarters(*(
                                pltpu.roll(
                                    lines[g], (blk * g + 8 * k) % LANES, axis=1, stride=1, stride_axis=0
                                )
                                for g in range(4)
                            )))
                        high, low = split(jnp.concatenate(tiles, axis=0))
                        at_row = pl.ds(LANES * q + 2 * blk * h, 2 * blk)
                        at_lane = pl.ds(LANES * half, LANES)
                        table[which, 0, at_row, at_lane] = high
                        table[which, 1, at_row, at_lane] = low

    def pack(tile):
        tall = jnp.concatenate([tile, pltpu.roll(tile, cols - 8, axis=1)], axis=0)
        pieces = [tall[:, k : k + LANES].T for k in range(0, cols, LANES)]
        form = jnp.concatenate(pieces, axis=0)
        return form.reshape(own_g, 2, 8, LANES)[:, 0]

    def expand(buf, tile, first, size):
        last = min(first + size, buf.shape[1] - 1)
        pk = buf[tile, first : first + size]
        after = buf[tile, last : last + 1]
        if size > 1:
            after = jnp.concatenate([pk[1:], after], axis=0)
        odd = jnp.where(low_half(pk), after, pk).reshape(-1, LANES)
        odd = turn(odd, LANES // 2).reshape(pk.shape)
        return jnp.stack([pk, odd], axis=1).reshape(size * 16, LANES)

    first_row, last_row = row == 0, row == n_row - 1
    left_on = jnp.where(col == 0, 0.0, 1.0)
    right_on = jnp.where(col == n_col - 1, 0.0, 1.0)

    def row_mask(at):
        off = jnp.logical_or(
            jnp.logical_and(at < 0, first_row), jnp.logical_and(at >= rows, last_row)
        )
        return jnp.where(off, 0.0, 1.0)

    def masked(value, start, margin, mask):
        out = []
        for j in range(start, start + value.shape[0], PIECE):
            piece = value[j - start : j - start + PIECE]
            side = mask
            if j < margin:
                side = mask * left_on
            elif j >= margin + cols:
                side = mask * right_on
            out.append(piece * side)
        return jnp.concatenate(out, axis=0) if len(out) > 1 else out[0]

    counters = {"piece": [0, 0], "stage": 0}

    def take(unit):
        acc = accs[unit][counters["piece"][unit] % PIECES]
        counters["piece"][unit] += 1
        return acc

    def put_window(slot, k, at, value):
        high, low = split(value)
        high_ref[slot, k, at : at + value.shape[0], :] = high
        low_ref[slot, k, at : at + value.shape[0], :] = low

    class Stage:
        def __init__(self, which, n, n_in, lag, emit, feed=None, before=None):
            self.which, self.n, self.n_in, self.emit, self.feed = which, n, n_in, emit, feed
            self.before = before
            self.slot = counters["stage"] % 2
            counters["stage"] += 1
            self.units, self.n_out = (n_in - 16) // PIECE, n_in - 32
            self.ends = [e for e in (step - lag for step in STEPS) if 0 < e < self.units] + [self.units]
            self.starts = [0] + self.ends[:-1]
            self.done_t = self.done_o = 0

        def cost(self, i):
            return self.n * ((self.ends[i] - self.starts[i] + 1) // 2) * 24

        def matmul(self, i):
            c0, c1, slot, n = self.starts[i], self.ends[i], self.slot, self.n
            if i == 0 and self.before is not None:
                self.before()
            if self.feed is not None:
                self.feed(slot, c1 * PIECE + PIECE)
            middle = (c0 + c1 + (i + 1) % 2) // 2
            share = (range(c0, middle), range(middle, c1))
            held = [[(k, u, take(unit)) for k in range(n) for u in share[unit]] for unit in range(2)]
            for part in range(2):
                for unit in range(2):
                    if held[unit]:
                        pltpu.matmul_push_rhs(
                            table[self.which, part], staging_register=part, mxu_index=unit
                        )
            for source, load in ((high_ref, 0), (low_ref, None), (high_ref, 1)):
                for unit in range(2):
                    for j, (k, u, acc) in enumerate(held[unit]):
                        at = PIECE * u
                        lhs = jnp.concatenate(
                            [source[slot, k, at : at + 16, :], source[slot, k, at + 16 : at + 32, :]], axis=1
                        )
                        pltpu.matmul_acc_lhs(acc, lhs, load_staged_rhs=load if j == 0 else None)
            self.held = held

        def pop(self):
            slot = self.slot
            for unit in range(2):
                for k, u, acc in self.held[unit]:
                    out = pltpu.matmul_pop(acc)
                    at = PIECE * u
                    wide[slot, 0, k, at : at + PIECE, :] = out[:, 0:LANES]
                    wide[slot, 1, k, at : at + PIECE, :] = out[:, LANES:]

        def vector(self, i):
            slot = self.slot
            rows_done = self.ends[i] * PIECE
            t0, t1 = self.done_t, rows_done - 8
            for k in range(self.n):
                partial_ref[slot, k, t0:t1, :] = wide[slot, 0, k, t0:t1, :] + wide[slot, 1, k, t0 + 4 : t1 + 4, :]
            self.done_t = t1
            o1 = min(rows_done - 16, self.n_out)
            o = self.done_o
            while o < o1:
                e = min(o - o % 32 + 32, o1)
                self.emit(1 - slot, o, e, functools.partial(taken, slot, o, e))
                o = e
            self.done_o = o1

    def pipeline(stages):
        lag = 540
        next_mm = [0] * len(stages)
        done = [[] for _ in stages]
        clock, pending = 0, []
        while any(n < len(st.ends) for n, st in zip(next_mm, stages)):
            options = []
            for s, st in enumerate(stages):
                i = next_mm[s]
                if i == len(st.ends):
                    continue
                ready = 0
                if s:
                    need = st.ends[i] + 3 if i + 1 < len(st.ends) else stages[s - 1].units
                    before = [t for e, t in zip(stages[s - 1].ends, done[s - 1]) if e >= need]
                    if not before:
                        continue
                    ready = before[0]
                options.append((max(ready, clock), s))
            start, s = min(options)
            st, i = stages[s], next_mm[s]
            for item in [p for p in pending if p[0] <= start]:
                item[1].vector(item[2])
                pending.remove(item)
            st.matmul(i)
            st.pop()
            next_mm[s] += 1
            clock = start + st.cost(i)
            done[s].append(clock + lag)
            pending.append((clock + 200, st, i))
        for item in pending:
            item[1].vector(item[2])

    def taken(slot, o, e, k, shift):
        return partial_ref[slot, k, o + shift : e + shift, :]

    def fold4(t, *source):
        out = 0.0
        for s in range(4):
            out = out + turn(quarters(*(t(source[(p + s) % 4], p) for p in range(4))), s * blk)
        return out

    class Windows:
        def __init__(self, n, blocks=False):
            self.n, self.blocks, self.kept, self.at = n, blocks, None, 0

        def make(self, slot, parts):
            size = parts[0].shape[0] - 16
            if self.blocks:
                for k in range(self.n):
                    a, b = parts[k], parts[k + 1]
                    win = quarters(a[0:size], b[0:size], a[8 : size + 8], b[8 : size + 8])
                    put_window(slot, k, self.at, win)
                self.at += size
                return
            value, t32, t64, t96, extra = parts

            def lo(x):
                return x[0:size]

            def hi(x):
                return x[8 : size + 8]

            for k in range(self.n):
                if k == 0:
                    win = jnp.where(low_half(lo(value)), lo(value), hi(t64))
                elif k == 1:
                    win = jnp.where(low_half(lo(value)), lo(t96), hi(t32))
                elif k == 2:
                    win = jnp.where(low_half(lo(value)), lo(t64), hi(value))
                else:
                    win = quarters(lo(t32), lo(extra), hi(t96), hi(extra))
                put_window(slot, k, self.at, win)
            self.at += size

        def add(self, slot, value, extra=None):
            if self.blocks:
                parts = value
            else:
                parts = [value, turn(value, blk), turn(value, 2 * blk), turn(value, 3 * blk), extra]
            if self.kept is not None:
                parts = [
                    None if new is None else jnp.concatenate([old, new], axis=0)
                    for old, new in zip(self.kept, parts)
                ]
            if parts[0].shape[0] > 16:
                self.make(slot, parts)
            self.kept = [None if p is None else p[p.shape[0] - 16 :] for p in parts]

        def end(self, slot):
            parts = [None if p is None else jnp.concatenate([p, p], axis=0) for p in self.kept]
            self.make(slot, parts)

    def smooth(index, start, end):
        center = state_ref[index, start:end, :]
        left = state_ref[index, start - 1 : end - 1, :]
        right = state_ref[index, start + 1 : end + 1, :]
        return PENALTY * (4.0 * center - turn(center, 1) - turn(center, -1) - left - right)

    def repack(buf, group, value):
        n = value.shape[0] // 16
        down, up = (turn(value, by).reshape(n, 2, 8, LANES) for by in (-16, 48))
        q = lanes_of((n, 8, LANES))
        lower = jnp.where(q < 16, up[:, 0], down[:, 0])
        upper = jnp.where(q < 80, down[:, 1], up[:, 1])
        buf[1, group : group + n] = jnp.where(q < 64, lower, upper)

    def swap(x):
        odd = lax.rem(lanes_of(x.shape) // blk, 2) == 1
        return jnp.where(odd, turn(x, blk), turn(x, -blk))

    class RolledFeed:
        def __init__(self, buf, first):
            self.buf, self.first, self.at = buf, first, 0

        def __call__(self, slot, upto):
            upto = min(upto, (self.buf.shape[1] - 2 * self.first) * 16)
            while self.at < upto:
                size = min(2, (upto - self.at) // 16)
                self.two(slot, self.first + self.at // 16, size)
                self.at += size * 16

        def two(self, slot, first, size):
            up, mid, down = (expand(self.buf, k, first, size) for k in range(3))
            at = self.at
            q = lax.rem(lanes_of(mid.shape), 2 * blk)
            second = jnp.where(q < 16, up, mid)
            fourth = jnp.where(q < 16, mid, down)
            start = swap(jnp.where(q < 16, up, jnp.where(q < blk, mid, up)))
            third = swap(jnp.where(jnp.logical_and(q >= 16, q < blk), down, mid))
            for k, w in enumerate((start, second, third, fourth)):
                put_window(slot, k, at, w)
            state_ref[0, at : at + size * 16, :] = jnp.where(
                low_half(mid), second, turn(fourth, 2 * blk)
            )

    class Feed:
        def __init__(self, buf, rolled):
            self.buf, self.rolled, self.at = buf, rolled, 0

        def __call__(self, slot, upto):
            upto = min(upto, self.buf.shape[1] * 16)
            while self.at < upto:
                self.two(slot, self.at // 16, min(2, (upto - self.at) // 16))

        def two(self, slot, first, size):
            up, mid, down = (expand(self.buf, s, first, size) for s in range(3))
            at = self.at
            if self.rolled:
                far = lax.rem(lanes_of(mid.shape), 2 * blk) >= 48
                up, mid, down = (jnp.where(far, turn(x, 48), turn(x, -16)) for x in (up, mid, down))
            odd = lax.rem(lanes_of(mid.shape), 2 * blk) >= blk
            upper = jnp.where(odd, turn(mid, blk), turn(up, -blk))
            lower = jnp.where(odd, turn(down, blk), turn(mid, -blk))
            for k, w in enumerate((up, upper, mid, lower, down)):
                put_window(slot, k, at, w)
            state_ref[0, at : at + size * 16, :] = jnp.where(low_half(mid), upper, turn(lower, 2 * blk))
            self.at += size * 16

    def tile_sum(x):
        return jnp.sum(x.reshape(-1, 8, LANES), axis=0)

    def collect(totals):
        line = jnp.zeros((1, LANES), jnp.float32)
        for k, x in enumerate(totals):
            x = jnp.sum(jnp.sum(x, axis=0, keepdims=True), axis=1, keepdims=True)
            line = jnp.where(lane1 == k, x, line)
        return line

    def red_copy(turn_no, place):
        return pltpu.make_async_remote_copy(
            src_ref=red.at[turn_no, me], dst_ref=red.at[turn_no, me],
            send_sem=red_send.at[turn_no], recv_sem=red_recv.at[turn_no],
            device_id=place, device_id_type=MESH,
        )

    def all_red(turn_no):
        return pltpu.make_async_remote_copy(
            src_ref=red.at[turn_no, pl.ds(0, count - 1)], dst_ref=red.at[turn_no, pl.ds(0, count - 1)],
            send_sem=red_send.at[turn_no], recv_sem=red_recv.at[turn_no],
            device_id=(row, col), device_id_type=MESH,
        )

    def flipped(x, n, bits):
        if n & (n - 1):
            return lax.rem(x + bits, n)
        for k in range(n.bit_length() - 1):
            if bits >> k & 1:
                x = x + (1 - 2 * lax.rem(x // (1 << k), 2)) * (1 << k)
        return x

    def spread(turn_no, line):
        red[turn_no, me] = line
        for r in reversed(range(n_row)):
            for c in reversed(range(n_col)):
                if r or c:
                    red_copy(turn_no, (flipped(row, n_row, r), flipped(col, n_col, c))).start()

    def gather(turn_no, n):
        all_red(turn_no).wait_recv()
        line = jnp.sum(red[turn_no], axis=0)
        return [
            jnp.sum(jnp.where(lane1 == k, line, 0.0), axis=1, keepdims=True) for k in range(n)
        ]

    right_groups = right_pack.shape[1]
    first_row_at, last_row_at = row == 0, row == n_row - 1

    def blank(where):
        right_pack[where] = jnp.zeros_like(right_pack[where])

    def right_form(half, s):
        x = right_ref[half * blk : half * blk + blk, :]
        tall = jnp.concatenate(
            [x if p == s else pltpu.roll(x, cols - 8 * ((p - s) % 4), axis=1) for p in range(4)], axis=0
        )
        pieces = [tall[:, k : k + LANES].T for k in range(0, cols, LANES)]
        return jnp.concatenate(pieces, axis=0).reshape(right_groups - 2, 4, 8, LANES)[:, 0]

    def each_right(act, sign):
        def one(index):
            dr, dc = DIRECTIONS[index]
            src, dst = {-1: (4, 3), 1: (5, 0), 0: (1, 1)}[dr]
            c_src, c_dst, c_len = (
                (1, right_groups - 1, 1) if dc < 0
                else (right_groups - 2, 0, 1) if dc > 0
                else (1, 1, right_groups - 2)
            )
            planes = 1 if dr else 2
            act(pltpu.make_async_remote_copy(
                src_ref=right_pack.at[pl.ds(src, planes), pl.ds(c_src, c_len)],
                dst_ref=right_pack.at[pl.ds(dst, planes), pl.ds(c_dst, c_len)],
                send_sem=send_sem.at[1, index],
                recv_sem=recv_sem.at[1, index],
                device_id=(row + dr, col + dc),
                device_id_type=MESH,
            ))

        for index, (dr, dc) in enumerate(DIRECTIONS):
            pl.when(inside(sign * dr, sign * dc))(functools.partial(one, index))

    def right_natural():
        each_right(lambda c: c.wait_recv(), -1)
        planes = [right_pack[k] for k in range(4)]
        for t in range(4):
            value = quarters(*(planes[(p - t) % 4].reshape(-1, LANES) for p in range(4)))
            right_nat[:, t] = turn(value, -blk * t).reshape(right_groups, 8, LANES)

    clear(first_pack)
    for at_edge, where in (
        (first_row_at, (slice(0, 1), slice(None))), (last_row_at, (slice(3, 4), slice(None))),
        (col == 0, (slice(0, 4), slice(0, 1))),
        (col == n_col - 1, (slice(0, 4), slice(right_groups - 1, right_groups))),
    ):
        pl.when(at_edge)(functools.partial(blank, where))
    clear(second_pack)
    edge1 = (first_pack.shape[1] - own_g) // 2
    edge2 = (second_pack.shape[1] - own_g) // 2
    loads[0].wait()
    first_pack[1, edge1 : edge1 + own_g] = pack(guess_ref[...])
    pl.semaphore_wait(barrier, heard(GREET))
    send(first_pack, 0)
    loads[1].wait()
    for plane, half, s in ((4, 0, 3), (5, 1, 0), (1, 0, 1), (2, 1, 2)):
        right_pack[plane, 1 : right_groups - 1] = right_form(half, s)
    each_right(lambda c: c.start(), 1)
    loads[2].wait()
    build_tables()

    mask48, mask32, mask16 = (row_mask(lane1 - k) for k in (48, 32, 16))
    mask_low = row_mask(rows + 16 + 0 * lane1)
    masks16 = [row_mask(blk * k - 16 + lax.rem(lane1, blk)) for k in range(3)]
    own32 = jnp.logical_and(lane1 >= 32, lane1 < 32 + rows)
    own16 = jnp.logical_and(lane1 >= 16, lane1 < 16 + rows)
    dots = [0.0] * SUMS
    first_sums = [0.0, 0.0]
    n_in = first_pack.shape[1] * 16

    def own_part(o, e, margin):
        a, b = max(o, margin), min(e, margin + cols)
        return slice(a - margin, b - margin), slice(a - o, b - o), a < b

    step = {}

    def late_wait():
        step["m0"], step["m1"] = gather(0, 2)
        step["alpha0"] = step["m0"] / step["m1"]

    def three_stages(buf, second):
        wins_b, wins_c, wins_d = Windows(4), Windows(3), Windows(2, True)

        def emit_a(slot, o, e, t):
            value = masked(fold4(t, 0, 1, 2, 3), o, 48, mask48)
            wins_b.add(slot, value, masked(fold4(t, 4, 4, 4, 4), o, 48, mask_low))
            if e == n_in - 32:
                wins_b.end(slot)

        def emit_b(slot, o, e, t):
            value = fold4(t, 0, 1, 2, 3) + smooth(0, o + 32, e + 32)
            if not second:
                value = right_nat[o // 32, :, :, :].reshape(32, LANES) - value if e - o == 32 else (
                    right_nat[o // 32, o % 32 // 8 : (o % 32 + e - o) // 8].reshape(e - o, LANES) - value
                )
            value = masked(value, o, 32, mask32)
            state_ref[1, o:e, :] = value
            wins_c.add(slot, value)
            if e == n_in - 64:
                wins_c.end(slot)

        def emit_c(slot, o, e, t):
            blocks = [masked(fold4(t, k, k, k, k), o, 16, masks16[k]) for k in range(3)]
            wins_d.add(slot, blocks)
            if e == n_in - 96:
                wins_d.end(slot)

        pipeline_of = [
            Stage(0, 5, n_in, 0, emit_a, Feed(buf, second)),
            Stage(1, 4, n_in - 32, 3, emit_b, before=None if second else right_natural),
            Stage(0, 3, n_in - 64, 6, emit_c),
        ]
        return pipeline_of

    def early_stages(buf):
        wins_f, wins_g = Windows(3), Windows(2)
        n_two = n_in - 32

        def emit_e(slot, o, e, t):
            value = masked(fold4(t, 0, 1, 2, 3), o, 32, mask32)
            to, of, some = own_part(o, e, 32)
            if some:
                own_ref[5, to, :] = value[of]
            wins_f.add(slot, value)
            if e == n_two - 32:
                wins_f.end(slot)

        def emit_f(slot, o, e, t):
            value = masked(fold4(t, 0, 1, 2, 2) + smooth(0, o + 32, e + 32), o, 16, mask16)
            state_ref[1, o:e, :] = value
            wins_g.add(slot, value)
            if e == n_two - 64:
                wins_g.end(slot)

        def emit_g(slot, o, e, t):
            if o == 32:
                products(step["alpha0"])
            value = jnp.where(own32, own_ref[5, o:e, :] - step["alpha0"] * fold4(t, 0, 0, 1, 1), 0.0)
            dots[8] += tile_sum(value * value)

        return [
            Stage(0, 4, n_two, 2, emit_e, RolledFeed(buf, 1)),
            Stage(1, 3, n_two - 32, 5, emit_f),
            Stage(0, 2, n_two - 64, 8, emit_g, before=late_wait),
        ]

    def products(alpha0):
        for o in range(0, cols, 32):
            e = o + 32
            r0 = own_ref[1, o:e, :]
            w1 = jnp.where(own16, state_ref[0, 48 + o : 48 + e, :], 0.0)
            w2 = jnp.where(own16, state_ref[1, 16 + o : 16 + e, :], 0.0)
            bend = smooth(0, 48 + o, 48 + e) - alpha0 * smooth(1, 16 + o, 16 + e)
            r1, q = r0 - alpha0 * w1, w1 - alpha0 * w2
            for k, x in ((2, w1), (3, w2), (4, q), (6, r1)):
                own_ref[k, o:e, :] = x
            for k, x in enumerate((r1 * r1, r1 * q, r1 * w1, w1 * w1, q * q, q * w1, q * w2, w1 * w2, q * bend)):
                dots[k] += tile_sum(x)

    rounds = greetings(n_row, n_col)
    receive(first_pack, 0)
    if rounds:
        greet(known_sem.at[0], rounds[0])
    def emit_d(slot, o, e, t):
        r0 = jnp.where(own32, state_ref[1, o + 32 : e + 32, :], 0.0)
        w1 = jnp.where(own32, fold4(t, 0, 0, 1, 1) + smooth(1, o + 32, e + 32), 0.0)
        repack(second_pack, edge2 + o // 16, w1)
        first_sums[0] += tile_sum(r0 * r0)
        first_sums[1] += tile_sum(r0 * w1)

    pipeline(three_stages(first_pack, False) + [Stage(1, 2, n_in - 96, 9, emit_d)])
    send(second_pack, 2)
    for k, offsets in enumerate(rounds):
        pl.semaphore_wait(known_sem.at[k], heard(offsets))
        if k + 1 < len(rounds):
            greet(known_sem.at[k + 1], rounds[k + 1])

    spread(0, collect(first_sums))
    finish(first_pack, 0)
    each_right(lambda c: c.wait_send(), 1)

    own_ref[1] = jnp.where(own16, turn(state_ref[1, 32 : 32 + cols, :], -16), 0.0)
    receive(second_pack, 2)
    pipeline(early_stages(second_pack))
    m0, m1, alpha0 = step["m0"], step["m1"], step["alpha0"]
    spread(1, collect(dots))
    finish(second_pack, 2)
    all_red(0).wait_send()

    def emit_h(slot, o, e, t):
        w3 = jnp.where(own32, fold4(t, 0, 0, 1, 1) + smooth(1, o + 32, e + 32), 0.0)
        w3 = turn(w3, -16)
        own_ref[5, o:e, :] = own_ref[3, o:e, :] - alpha0 * w3

    pipeline(three_stages(second_pack, True) + [Stage(1, 2, n_in - 96, 9, emit_h)])

    def upright(k):
        return jnp.concatenate(
            [own_ref[k, j : j + LANES, :].T[16 : 16 + rows] for j in range(0, cols, LANES)], axis=1
        )

    shared_ref[...] = upright(6)
    for at, k in enumerate((1, 2, 3, 4, 5)):
        upright_ref[at] = upright(k)

    rr1, r1q, r1w, ww, qq, qw, qw2, ww2, qaq = gather(1, SUMS)
    beta0 = rr1 / m0
    alpha1 = rr1 / (r1q + beta0 * (2.0 * r1w + beta0 * m1))
    both = alpha1 * beta0
    rr2 = rr1 - 2.0 * alpha1 * (r1q + beta0 * r1w) + alpha1 * alpha1 * (
        qq + beta0 * (2.0 * qw + beta0 * ww)
    )
    beta1 = rr2 / rr1
    r2ar2 = (
        r1q + alpha1 * alpha1 * qaq + both * both * ww2
        - 2.0 * alpha1 * qq - 2.0 * both * qw + 2.0 * alpha1 * both * qw2
    )
    alpha2 = rr2 / (r2ar2 - beta1 * rr2 / alpha1)
    t_r0 = alpha0 + both + alpha2 * beta1 * beta0
    t_r1 = alpha1 + alpha2 * (1.0 + beta1)
    t_q, t_w1 = -alpha2 * alpha1, -alpha2 * both
    s_q, s_w1 = -alpha1 - alpha2 * (1.0 + beta1), -both - alpha2 * beta1 * beta0
    s_aq, s_w2 = alpha2 * alpha1, alpha2 * both
    r0, w1, w2, q, aq = (upright_ref[k] for k in range(5))
    template_ref[...] = guess_ref[...] + t_r0 * r0 + (t_r1 - 1.0) * shared_ref[...] + t_q * q + t_w1 * w1
    residual_ref[...] = s_q * q + s_w1 * w1 + s_aq * aq + s_w2 * w2
    all_red(1).wait_send()


def on_device(n_row, n_col, right_side, initial_guess, kernel):
    rows, cols = right_side.shape
    count = n_row * n_col
    shape = pltpu.VMEM((rows, cols), jnp.float32)
    f32, bf16 = jnp.float32, jnp.bfloat16
    tall = cols + 2 * rows
    packs = [pltpu.VMEM((3, cols // 16 + 2 * (rows // 16), 8, LANES), f32) for _ in range(2)]
    packs.insert(1, pltpu.VMEM((6, cols // 32 + 2, 8, LANES), f32))
    template, residual, shared = pl.pallas_call(
        functools.partial(body, n_row, n_col),
        out_shape=(shape,) * 3,
        in_specs=[pl.BlockSpec(memory_space=pl.ANY)] * 3,
        out_specs=[pl.BlockSpec(memory_space=pltpu.VMEM)] * 3,
        scratch_shapes=[
            pltpu.VMEM((rows, cols), f32),
            pltpu.VMEM((rows, cols), f32),
            pltpu.VMEM(kernel.shape, f32),
            *packs,
            pltpu.VMEM((2, LANES, LANES), f32),
            pltpu.VMEM((2, 2, 2 * LANES, 2 * LANES), bf16),
            pltpu.VMEM((2, 5, tall, LANES), bf16),
            pltpu.VMEM((2, 5, tall, LANES), bf16),
            pltpu.VMEM((2, 2, 5, tall, LANES), f32),
            pltpu.VMEM((2, 5, tall, LANES), f32),
            pltpu.VMEM((2, tall, LANES), f32),
            pltpu.VMEM((cols // 32 + 2, 4, 8, LANES), f32),
            pltpu.VMEM((7, cols, LANES), f32),
            pltpu.VMEM((5, rows, cols), f32),
            pltpu.VMEM((2, count, 1, LANES), f32),
            pltpu.SemaphoreType.DMA((3,)),
            pltpu.SemaphoreType.DMA((3, len(DIRECTIONS))),
            pltpu.SemaphoreType.DMA((3, len(DIRECTIONS))),
            pltpu.SemaphoreType.DMA((2,)),
            pltpu.SemaphoreType.DMA((2,)),
            pltpu.SemaphoreType.REGULAR((len(greetings(n_row, n_col)),)),
        ],
        compiler_params=pltpu.CompilerParams(collective_id=0, has_side_effects=True),
    )(right_side, initial_guess, kernel)
    return template + shared, residual + shared


def solution(mesh):
    placed = (P("row", "col"), P("row", "col"), P())
    return jax.shard_map(
        functools.partial(on_device, mesh.shape["row"], mesh.shape["col"]),
        mesh=mesh,
        in_specs=placed,
        out_specs=(P("row", "col"), P("row", "col")),
        check_vma=False,
    )
```

```python
import functools

import jax
import jax.numpy as jnp
from jax import lax
from jax.experimental import pallas as pl
from jax.experimental.pallas import tpu as pltpu
from jax.sharding import PartitionSpec as P

PENALTY = 0.05
LANES = 128
PIECE = 16
PIECES = 64
STEPS = (8, 15, 20)
SUMS = 9
MESH = pl.DeviceIdType.MESH
DIRECTIONS = ((-1, -1), (-1, 1), (1, -1), (1, 1), (-1, 0), (1, 0), (0, -1), (0, 1))


NEAR = tuple((a, b) for a in (-1, 0, 1) for b in (-1, 0, 1) if (a, b) != (0, 0))
GREET = tuple(sorted(NEAR, key=lambda p: -abs(p[0]) - abs(p[1]))) + ((0, -4), (0, 4))


def square(r, c):
    return tuple((a, b) for a in (-r, 0, r) for b in (-c, 0, c) if (a, b) != (0, 0))


def greetings(n_row, n_col):
    places = [(r, c) for r in range(n_row) for c in range(n_col)]

    def reach(place, offsets):
        near = ((place[0] + a, place[1] + b) for a, b in offsets)
        return [p for p in near if 0 <= p[0] < n_row and 0 <= p[1] < n_col]

    def hear(known, offsets):
        if any(p not in known[d] for d in places for p in reach(d, offsets)):
            return None
        return {d: known[d].union(*(known[p] for p in reach(d, offsets))) for d in places}

    known = {d: {d, *reach(d, GREET)} for d in places}
    known = hear(known, NEAR)
    rounds = []
    while min(map(len, known.values())) < len(places):
        best = None
        for r in range(1, max(2, n_row)):
            for c in range(1, max(2, n_col)):
                after = hear(known, square(r, c))
                if after is not None:
                    score = (min(map(len, after.values())), -r - c)
                    if best is None or score > best[0]:
                        best = (score, square(r, c), after)
        rounds.append(best[1])
        known = best[2]
    return rounds


def split(x):
    high = x.astype(jnp.bfloat16)
    low = (x - high.astype(jnp.float32)).astype(jnp.bfloat16)
    return high, low


def body(n_row, n_col, *refs):
    pieces = [
        pltpu.ACC(unit)((PIECE, 2 * LANES), jnp.float32) for unit in range(2) for _ in range(PIECES)
    ]

    def inner(*accs):
        run(n_row, n_col, (accs[:PIECES], accs[PIECES:]), *refs)

    pl.run_scoped(inner, *pieces)


def run(
    n_row, n_col, accs,
    right_hbm, guess_hbm, kernel_hbm, template_ref, residual_ref, shared_ref,
    right_ref, guess_ref, kernel_ref, first_pack, right_pack, second_pack,
    lines_ref, table, high_ref, low_ref, wide, partial_ref,
    state_ref, right_nat, own_ref, upright_ref, red, load_sem, send_sem, recv_sem, red_send, red_recv, known_sem,
):
    rows, cols = right_ref.shape
    row, col = lax.axis_index("row"), lax.axis_index("col")
    me, count = row * n_col + col, n_row * n_col
    width = kernel_ref.shape[0]
    blk = rows // 2
    own_g = cols // PIECE

    barrier = pltpu.get_barrier_semaphore()

    def within(dr, dc):
        return jnp.logical_and(
            jnp.logical_and(row + dr >= 0, row + dr < n_row),
            jnp.logical_and(col + dc >= 0, col + dc < n_col),
        )

    def greet(sem, offsets):
        for dr, dc in offsets:
            pl.when(within(dr, dc))(
                lambda dr=dr, dc=dc: pl.semaphore_signal(
                    sem, inc=1, device_id=(row + dr, col + dc), device_id_type=MESH
                )
            )

    def heard(offsets):
        return functools.reduce(jnp.add, [jnp.where(within(dr, dc), 1, 0) for dr, dc in offsets])

    greet(barrier, GREET)
    loads = [
        pltpu.make_async_copy(src, dst, load_sem.at[k])
        for k, (src, dst) in enumerate(
            ((guess_hbm, guess_ref), (right_hbm, right_ref), (kernel_hbm, kernel_ref))
        )
    ]
    for load in loads:
        load.start()

    lane1 = lax.broadcasted_iota(jnp.int32, (1, LANES), 1)

    def lanes_of(shape):
        return lax.broadcasted_iota(jnp.int32, shape, len(shape) - 1)

    def low_half(x):
        return lanes_of(x.shape) < LANES // 2

    def quarters(a, b, c, d):
        q = lanes_of(a.shape)
        return jnp.where(
            q < 2 * blk, jnp.where(q < blk, a, b), jnp.where(q < 3 * blk, c, d)
        )

    def turn(x, by):
        return pltpu.roll(x, by % LANES, axis=1)

    def inside(dr, dc):
        checks = []
        if dr:
            checks.append(row + dr >= 0 if dr < 0 else row + dr < n_row)
        if dc:
            checks.append(col + dc >= 0 if dc < 0 else col + dc < n_col)
        return functools.reduce(jnp.logical_and, checks)

    def clear(buf):
        groups = buf.shape[1]
        edge = (groups - own_g) // 2

        @pl.when(row == 0)
        def _():
            buf[0] = jnp.zeros(buf.shape[1:], jnp.float32)

        @pl.when(row == n_row - 1)
        def _():
            buf[2] = jnp.zeros(buf.shape[1:], jnp.float32)

        @pl.when(col == 0)
        def _():
            buf[:, 0:edge] = jnp.zeros((3, edge, 8, LANES), jnp.float32)

        @pl.when(col == n_col - 1)
        def _():
            buf[:, groups - edge : groups] = jnp.zeros((3, edge, 8, LANES), jnp.float32)

    def each(buf, turn_no, act, sign):
        groups = buf.shape[1]
        edge = (groups - own_g) // 2

        def one(index):
            dr, dc = DIRECTIONS[index]
            c_src, c_dst, c_len = (
                (edge, groups - edge, edge) if dc < 0
                else (own_g, 0, edge) if dc > 0
                else (edge, edge, own_g)
            )
            act(pltpu.make_async_remote_copy(
                src_ref=buf.at[1, pl.ds(c_src, c_len)],
                dst_ref=buf.at[1 - dr, pl.ds(c_dst, c_len)],
                send_sem=send_sem.at[turn_no, index],
                recv_sem=recv_sem.at[turn_no, index],
                device_id=(row + dr, col + dc),
                device_id_type=MESH,
            ))

        for index, (dr, dc) in enumerate(DIRECTIONS):
            pl.when(inside(sign * dr, sign * dc))(functools.partial(one, index))

    def send(buf, turn_no):
        each(buf, turn_no, lambda c: c.start(), 1)

    def receive(buf, turn_no):
        each(buf, turn_no, lambda c: c.wait_recv(), -1)

    def finish(buf, turn_no):
        each(buf, turn_no, lambda c: c.wait_send(), 1)

    def flip(x):
        return jnp.concatenate([x[a : a + 1] for a in reversed(range(width))] + [x[width:]], axis=0)

    def build_tables():
        taps = kernel_ref[...]
        taps = jnp.concatenate([taps, jnp.zeros((width, LANES - width), jnp.float32)], axis=1)
        taps = jnp.concatenate([taps, jnp.zeros((LANES - width, LANES), jnp.float32)], axis=0)
        lines_ref[0] = turn(flip(taps).T, -width)
        lines_ref[1] = turn(taps.T, -width)

        for which in range(2):
            for q in range(2):
                for h in range(2):
                    for half in range(2):
                        lines = []
                        for g in range(4):
                            b = 16 * q + 8 * h + 4 * half + g
                            source = b - 1 if which == 0 else width - b
                            if b == 0:
                                lines.append(jnp.zeros((8, LANES), jnp.float32))
                            else:
                                lines.append(
                                    jnp.broadcast_to(lines_ref[which, source : source + 1, :], (8, LANES))
                                )
                        tiles = []
                        for k in range(2 * blk // 8):
                            tiles.append(quarters(*(
                                pltpu.roll(
                                    lines[g], (blk * g + 8 * k) % LANES, axis=1, stride=1, stride_axis=0
                                )
                                for g in range(4)
                            )))
                        high, low = split(jnp.concatenate(tiles, axis=0))
                        at_row = pl.ds(LANES * q + 2 * blk * h, 2 * blk)
                        at_lane = pl.ds(LANES * half, LANES)
                        table[which, 0, at_row, at_lane] = high
                        table[which, 1, at_row, at_lane] = low

    def pack(tile):
        tall = jnp.concatenate([tile, pltpu.roll(tile, cols - 8, axis=1)], axis=0)
        pieces = [tall[:, k : k + LANES].T for k in range(0, cols, LANES)]
        form = jnp.concatenate(pieces, axis=0)
        return form.reshape(own_g, 2, 8, LANES)[:, 0]

    def expand(buf, tile, first, size):
        last = min(first + size, buf.shape[1] - 1)
        pk = buf[tile, first : first + size]
        after = buf[tile, last : last + 1]
        if size > 1:
            after = jnp.concatenate([pk[1:], after], axis=0)
        odd = jnp.where(low_half(pk), after, pk).reshape(-1, LANES)
        odd = turn(odd, LANES // 2).reshape(pk.shape)
        return jnp.stack([pk, odd], axis=1).reshape(size * 16, LANES)

    first_row, last_row = row == 0, row == n_row - 1
    left_on = jnp.where(col == 0, 0.0, 1.0)
    right_on = jnp.where(col == n_col - 1, 0.0, 1.0)

    def row_mask(at):
        off = jnp.logical_or(
            jnp.logical_and(at < 0, first_row), jnp.logical_and(at >= rows, last_row)
        )
        return jnp.where(off, 0.0, 1.0)

    def masked(value, start, margin, mask):
        out = []
        for j in range(start, start + value.shape[0], PIECE):
            piece = value[j - start : j - start + PIECE]
            side = mask
            if j < margin:
                side = mask * left_on
            elif j >= margin + cols:
                side = mask * right_on
            out.append(piece * side)
        return jnp.concatenate(out, axis=0) if len(out) > 1 else out[0]

    counters = {"piece": [0, 0], "stage": 0}

    def take(unit):
        acc = accs[unit][counters["piece"][unit] % PIECES]
        counters["piece"][unit] += 1
        return acc

    def put_window(slot, k, at, value):
        high, low = split(value)
        high_ref[slot, k, at : at + value.shape[0], :] = high
        low_ref[slot, k, at : at + value.shape[0], :] = low

    class Stage:
        def __init__(self, which, n, n_in, lag, emit, feed=None, before=None):
            self.which, self.n, self.n_in, self.emit, self.feed = which, n, n_in, emit, feed
            self.before = before
            self.slot = counters["stage"] % 2
            counters["stage"] += 1
            self.units, self.n_out = (n_in - 16) // PIECE, n_in - 32
            self.ends = [e for e in (step - lag for step in STEPS) if 0 < e < self.units] + [self.units]
            self.starts = [0] + self.ends[:-1]
            self.done_t = self.done_o = 0

        def cost(self, i):
            return self.n * ((self.ends[i] - self.starts[i] + 1) // 2) * 24

        def matmul(self, i):
            c0, c1, slot, n = self.starts[i], self.ends[i], self.slot, self.n
            if i == 0 and self.before is not None:
                self.before()
            if self.feed is not None:
                self.feed(slot, c1 * PIECE + PIECE)
            middle = (c0 + c1 + (i + 1) % 2) // 2
            share = (range(c0, middle), range(middle, c1))
            held = [[(k, u, take(unit)) for k in range(n) for u in share[unit]] for unit in range(2)]
            for part in range(2):
                for unit in range(2):
                    if held[unit]:
                        pltpu.matmul_push_rhs(
                            table[self.which, part], staging_register=part, mxu_index=unit
                        )
            for source, load in ((high_ref, 0), (low_ref, None), (high_ref, 1)):
                for unit in range(2):
                    for j, (k, u, acc) in enumerate(held[unit]):
                        at = PIECE * u
                        lhs = jnp.concatenate(
                            [source[slot, k, at : at + 16, :], source[slot, k, at + 16 : at + 32, :]], axis=1
                        )
                        pltpu.matmul_acc_lhs(acc, lhs, load_staged_rhs=load if j == 0 else None)
            self.held = held

        def pop(self):
            slot = self.slot
            for unit in range(2):
                for k, u, acc in self.held[unit]:
                    out = pltpu.matmul_pop(acc)
                    at = PIECE * u
                    wide[slot, 0, k, at : at + PIECE, :] = out[:, 0:LANES]
                    wide[slot, 1, k, at : at + PIECE, :] = out[:, LANES:]

        def vector(self, i):
            slot = self.slot
            rows_done = self.ends[i] * PIECE
            t0, t1 = self.done_t, rows_done - 8
            for k in range(self.n):
                partial_ref[slot, k, t0:t1, :] = wide[slot, 0, k, t0:t1, :] + wide[slot, 1, k, t0 + 4 : t1 + 4, :]
            self.done_t = t1
            o1 = min(rows_done - 16, self.n_out)
            o = self.done_o
            while o < o1:
                e = min(o - o % 32 + 32, o1)
                self.emit(1 - slot, o, e, functools.partial(taken, slot, o, e))
                o = e
            self.done_o = o1

    def pipeline(stages):
        lag = 540
        next_mm = [0] * len(stages)
        done = [[] for _ in stages]
        clock, pending = 0, []
        while any(n < len(st.ends) for n, st in zip(next_mm, stages)):
            options = []
            for s, st in enumerate(stages):
                i = next_mm[s]
                if i == len(st.ends):
                    continue
                ready = 0
                if s:
                    need = st.ends[i] + 3 if i + 1 < len(st.ends) else stages[s - 1].units
                    before = [t for e, t in zip(stages[s - 1].ends, done[s - 1]) if e >= need]
                    if not before:
                        continue
                    ready = before[0]
                options.append((max(ready, clock), s))
            start, s = min(options)
            st, i = stages[s], next_mm[s]
            for item in [p for p in pending if p[0] <= start]:
                item[1].vector(item[2])
                pending.remove(item)
            st.matmul(i)
            st.pop()
            next_mm[s] += 1
            clock = start + st.cost(i)
            done[s].append(clock + lag)
            pending.append((clock + 200, st, i))
        for item in pending:
            item[1].vector(item[2])

    def taken(slot, o, e, k, shift):
        return partial_ref[slot, k, o + shift : e + shift, :]

    def fold4(t, *source):
        out = 0.0
        for s in range(4):
            out = out + turn(quarters(*(t(source[(p + s) % 4], p) for p in range(4))), s * blk)
        return out

    class Windows:
        def __init__(self, n, blocks=False):
            self.n, self.blocks, self.kept, self.at = n, blocks, None, 0

        def make(self, slot, parts):
            size = parts[0].shape[0] - 16
            if self.blocks:
                for k in range(self.n):
                    a, b = parts[k], parts[k + 1]
                    win = quarters(a[0:size], b[0:size], a[8 : size + 8], b[8 : size + 8])
                    put_window(slot, k, self.at, win)
                self.at += size
                return
            value, t32, t64, t96, extra = parts

            def lo(x):
                return x[0:size]

            def hi(x):
                return x[8 : size + 8]

            for k in range(self.n):
                if k == 0:
                    win = jnp.where(low_half(lo(value)), lo(value), hi(t64))
                elif k == 1:
                    win = jnp.where(low_half(lo(value)), lo(t96), hi(t32))
                elif k == 2:
                    win = jnp.where(low_half(lo(value)), lo(t64), hi(value))
                else:
                    win = quarters(lo(t32), lo(extra), hi(t96), hi(extra))
                put_window(slot, k, self.at, win)
            self.at += size

        def add(self, slot, value, extra=None):
            if self.blocks:
                parts = value
            else:
                parts = [value, turn(value, blk), turn(value, 2 * blk), turn(value, 3 * blk), extra]
            if self.kept is not None:
                parts = [
                    None if new is None else jnp.concatenate([old, new], axis=0)
                    for old, new in zip(self.kept, parts)
                ]
            if parts[0].shape[0] > 16:
                self.make(slot, parts)
            self.kept = [None if p is None else p[p.shape[0] - 16 :] for p in parts]

        def end(self, slot):
            parts = [None if p is None else jnp.concatenate([p, p], axis=0) for p in self.kept]
            self.make(slot, parts)

    def smooth(index, start, end):
        center = state_ref[index, start:end, :]
        left = state_ref[index, start - 1 : end - 1, :]
        right = state_ref[index, start + 1 : end + 1, :]
        return PENALTY * (4.0 * center - turn(center, 1) - turn(center, -1) - left - right)

    def repack(buf, group, value):
        n = value.shape[0] // 16
        down, up = (turn(value, by).reshape(n, 2, 8, LANES) for by in (-16, 48))
        q = lanes_of((n, 8, LANES))
        lower = jnp.where(q < 16, up[:, 0], down[:, 0])
        upper = jnp.where(q < 80, down[:, 1], up[:, 1])
        buf[1, group : group + n] = jnp.where(q < 64, lower, upper)

    def swap(x):
        odd = lax.rem(lanes_of(x.shape) // blk, 2) == 1
        return jnp.where(odd, turn(x, blk), turn(x, -blk))

    class RolledFeed:
        def __init__(self, buf, first):
            self.buf, self.first, self.at = buf, first, 0

        def __call__(self, slot, upto):
            upto = min(upto, (self.buf.shape[1] - 2 * self.first) * 16)
            while self.at < upto:
                size = min(2, (upto - self.at) // 16)
                self.two(slot, self.first + self.at // 16, size)
                self.at += size * 16

        def two(self, slot, first, size):
            up, mid, down = (expand(self.buf, k, first, size) for k in range(3))
            at = self.at
            q = lax.rem(lanes_of(mid.shape), 2 * blk)
            second = jnp.where(q < 16, up, mid)
            fourth = jnp.where(q < 16, mid, down)
            start = swap(jnp.where(q < 16, up, jnp.where(q < blk, mid, up)))
            third = swap(jnp.where(jnp.logical_and(q >= 16, q < blk), down, mid))
            for k, w in enumerate((start, second, third, fourth)):
                put_window(slot, k, at, w)
            state_ref[0, at : at + size * 16, :] = jnp.where(
                low_half(mid), second, turn(fourth, 2 * blk)
            )

    class Feed:
        def __init__(self, buf, rolled):
            self.buf, self.rolled, self.at = buf, rolled, 0

        def __call__(self, slot, upto):
            upto = min(upto, self.buf.shape[1] * 16)
            while self.at < upto:
                self.two(slot, self.at // 16, min(2, (upto - self.at) // 16))

        def two(self, slot, first, size):
            up, mid, down = (expand(self.buf, s, first, size) for s in range(3))
            at = self.at
            if self.rolled:
                far = lax.rem(lanes_of(mid.shape), 2 * blk) >= 48
                up, mid, down = (jnp.where(far, turn(x, 48), turn(x, -16)) for x in (up, mid, down))
            odd = lax.rem(lanes_of(mid.shape), 2 * blk) >= blk
            upper = jnp.where(odd, turn(mid, blk), turn(up, -blk))
            lower = jnp.where(odd, turn(down, blk), turn(mid, -blk))
            for k, w in enumerate((up, upper, mid, lower, down)):
                put_window(slot, k, at, w)
            state_ref[0, at : at + size * 16, :] = jnp.where(low_half(mid), upper, turn(lower, 2 * blk))
            self.at += size * 16

    def tile_sum(x):
        return jnp.sum(x.reshape(-1, 8, LANES), axis=0)

    def collect(totals):
        line = jnp.zeros((1, LANES), jnp.float32)
        for k, x in enumerate(totals):
            x = jnp.sum(jnp.sum(x, axis=0, keepdims=True), axis=1, keepdims=True)
            line = jnp.where(lane1 == k, x, line)
        return line

    def red_copy(turn_no, place):
        return pltpu.make_async_remote_copy(
            src_ref=red.at[turn_no, me], dst_ref=red.at[turn_no, me],
            send_sem=red_send.at[turn_no], recv_sem=red_recv.at[turn_no],
            device_id=place, device_id_type=MESH,
        )

    def all_red(turn_no):
        return pltpu.make_async_remote_copy(
            src_ref=red.at[turn_no, pl.ds(0, count - 1)], dst_ref=red.at[turn_no, pl.ds(0, count - 1)],
            send_sem=red_send.at[turn_no], recv_sem=red_recv.at[turn_no],
            device_id=(row, col), device_id_type=MESH,
        )

    def flipped(x, n, bits):
        if n & (n - 1):
            return lax.rem(x + bits, n)
        for k in range(n.bit_length() - 1):
            if bits >> k & 1:
                x = x + (1 - 2 * lax.rem(x // (1 << k), 2)) * (1 << k)
        return x

    def spread(turn_no, line):
        red[turn_no, me] = line
        for r in reversed(range(n_row)):
            for c in reversed(range(n_col)):
                if r or c:
                    red_copy(turn_no, (flipped(row, n_row, r), flipped(col, n_col, c))).start()

    def gather(turn_no, n):
        all_red(turn_no).wait_recv()
        line = jnp.sum(red[turn_no], axis=0)
        return [
            jnp.sum(jnp.where(lane1 == k, line, 0.0), axis=1, keepdims=True) for k in range(n)
        ]

    right_groups = right_pack.shape[1]
    first_row_at, last_row_at = row == 0, row == n_row - 1

    def blank(where):
        right_pack[where] = jnp.zeros_like(right_pack[where])

    def right_form(half, s):
        x = right_ref[half * blk : half * blk + blk, :]
        tall = jnp.concatenate(
            [x if p == s else pltpu.roll(x, cols - 8 * ((p - s) % 4), axis=1) for p in range(4)], axis=0
        )
        pieces = [tall[:, k : k + LANES].T for k in range(0, cols, LANES)]
        return jnp.concatenate(pieces, axis=0).reshape(right_groups - 2, 4, 8, LANES)[:, 0]

    def each_right(act, sign):
        def one(index):
            dr, dc = DIRECTIONS[index]
            src, dst = {-1: (4, 3), 1: (5, 0), 0: (1, 1)}[dr]
            c_src, c_dst, c_len = (
                (1, right_groups - 1, 1) if dc < 0
                else (right_groups - 2, 0, 1) if dc > 0
                else (1, 1, right_groups - 2)
            )
            planes = 1 if dr else 2
            act(pltpu.make_async_remote_copy(
                src_ref=right_pack.at[pl.ds(src, planes), pl.ds(c_src, c_len)],
                dst_ref=right_pack.at[pl.ds(dst, planes), pl.ds(c_dst, c_len)],
                send_sem=send_sem.at[1, index],
                recv_sem=recv_sem.at[1, index],
                device_id=(row + dr, col + dc),
                device_id_type=MESH,
            ))

        for index, (dr, dc) in enumerate(DIRECTIONS):
            pl.when(inside(sign * dr, sign * dc))(functools.partial(one, index))

    def right_natural():
        each_right(lambda c: c.wait_recv(), -1)
        planes = [right_pack[k] for k in range(4)]
        for t in range(4):
            value = quarters(*(planes[(p - t) % 4].reshape(-1, LANES) for p in range(4)))
            right_nat[:, t] = turn(value, -blk * t).reshape(right_groups, 8, LANES)

    clear(first_pack)
    for at_edge, where in (
        (first_row_at, (slice(0, 1), slice(None))), (last_row_at, (slice(3, 4), slice(None))),
        (col == 0, (slice(0, 4), slice(0, 1))),
        (col == n_col - 1, (slice(0, 4), slice(right_groups - 1, right_groups))),
    ):
        pl.when(at_edge)(functools.partial(blank, where))
    clear(second_pack)
    edge1 = (first_pack.shape[1] - own_g) // 2
    edge2 = (second_pack.shape[1] - own_g) // 2
    loads[0].wait()
    first_pack[1, edge1 : edge1 + own_g] = pack(guess_ref[...])
    pl.semaphore_wait(barrier, heard(GREET))
    send(first_pack, 0)
    loads[1].wait()
    for plane, half, s in ((4, 0, 3), (5, 1, 0), (1, 0, 1), (2, 1, 2)):
        right_pack[plane, 1 : right_groups - 1] = right_form(half, s)
    each_right(lambda c: c.start(), 1)
    loads[2].wait()
    build_tables()

    mask48, mask32, mask16 = (row_mask(lane1 - k) for k in (48, 32, 16))
    mask_low = row_mask(rows + 16 + 0 * lane1)
    masks16 = [row_mask(blk * k - 16 + lax.rem(lane1, blk)) for k in range(3)]
    own32 = jnp.logical_and(lane1 >= 32, lane1 < 32 + rows)
    own16 = jnp.logical_and(lane1 >= 16, lane1 < 16 + rows)
    dots = [0.0] * SUMS
    first_sums = [0.0, 0.0]
    n_in = first_pack.shape[1] * 16

    def own_part(o, e, margin):
        a, b = max(o, margin), min(e, margin + cols)
        return slice(a - margin, b - margin), slice(a - o, b - o), a < b

    step = {}

    def late_wait():
        step["m0"], step["m1"] = gather(0, 2)
        step["alpha0"] = step["m0"] / step["m1"]

    def three_stages(buf, second):
        wins_b, wins_c, wins_d = Windows(4), Windows(3), Windows(2, True)

        def emit_a(slot, o, e, t):
            value = masked(fold4(t, 0, 1, 2, 3), o, 48, mask48)
            wins_b.add(slot, value, masked(fold4(t, 4, 4, 4, 4), o, 48, mask_low))
            if e == n_in - 32:
                wins_b.end(slot)

        def emit_b(slot, o, e, t):
            value = fold4(t, 0, 1, 2, 3) + smooth(0, o + 32, e + 32)
            if not second:
                value = right_nat[o // 32, :, :, :].reshape(32, LANES) - value if e - o == 32 else (
                    right_nat[o // 32, o % 32 // 8 : (o % 32 + e - o) // 8].reshape(e - o, LANES) - value
                )
            value = masked(value, o, 32, mask32)
            state_ref[1, o:e, :] = value
            wins_c.add(slot, value)
            if e == n_in - 64:
                wins_c.end(slot)

        def emit_c(slot, o, e, t):
            blocks = [masked(fold4(t, k, k, k, k), o, 16, masks16[k]) for k in range(3)]
            wins_d.add(slot, blocks)
            if e == n_in - 96:
                wins_d.end(slot)

        pipeline_of = [
            Stage(0, 5, n_in, 0, emit_a, Feed(buf, second)),
            Stage(1, 4, n_in - 32, 3, emit_b, before=None if second else right_natural),
            Stage(0, 3, n_in - 64, 6, emit_c),
        ]
        return pipeline_of

    def early_stages(buf):
        wins_f, wins_g = Windows(3), Windows(2)
        n_two = n_in - 32

        def emit_e(slot, o, e, t):
            value = masked(fold4(t, 0, 1, 2, 3), o, 32, mask32)
            to, of, some = own_part(o, e, 32)
            if some:
                own_ref[5, to, :] = value[of]
            wins_f.add(slot, value)
            if e == n_two - 32:
                wins_f.end(slot)

        def emit_f(slot, o, e, t):
            value = masked(fold4(t, 0, 1, 2, 2) + smooth(0, o + 32, e + 32), o, 16, mask16)
            state_ref[1, o:e, :] = value
            wins_g.add(slot, value)
            if e == n_two - 64:
                wins_g.end(slot)

        def emit_g(slot, o, e, t):
            if o == 32:
                products(step["alpha0"])
            value = jnp.where(own32, own_ref[5, o:e, :] - step["alpha0"] * fold4(t, 0, 0, 1, 1), 0.0)
            dots[8] += tile_sum(value * value)

        return [
            Stage(0, 4, n_two, 2, emit_e, RolledFeed(buf, 1)),
            Stage(1, 3, n_two - 32, 5, emit_f),
            Stage(0, 2, n_two - 64, 8, emit_g, before=late_wait),
        ]

    def products(alpha0):
        for o in range(0, cols, 32):
            e = o + 32
            r0 = own_ref[1, o:e, :]
            w1 = jnp.where(own16, state_ref[0, 48 + o : 48 + e, :], 0.0)
            w2 = jnp.where(own16, state_ref[1, 16 + o : 16 + e, :], 0.0)
            bend = smooth(0, 48 + o, 48 + e) - alpha0 * smooth(1, 16 + o, 16 + e)
            r1, q = r0 - alpha0 * w1, w1 - alpha0 * w2
            for k, x in ((2, w1), (3, w2), (4, q), (6, r1)):
                own_ref[k, o:e, :] = x
            for k, x in enumerate((r1 * r1, r1 * q, r1 * w1, w1 * w1, q * q, q * w1, q * w2, w1 * w2, q * bend)):
                dots[k] += tile_sum(x)

    rounds = greetings(n_row, n_col)
    receive(first_pack, 0)
    if rounds:
        greet(known_sem.at[0], rounds[0])
    def emit_d(slot, o, e, t):
        r0 = jnp.where(own32, state_ref[1, o + 32 : e + 32, :], 0.0)
        w1 = jnp.where(own32, fold4(t, 0, 0, 1, 1) + smooth(1, o + 32, e + 32), 0.0)
        repack(second_pack, edge2 + o // 16, w1)
        first_sums[0] += tile_sum(r0 * r0)
        first_sums[1] += tile_sum(r0 * w1)

    pipeline(three_stages(first_pack, False) + [Stage(1, 2, n_in - 96, 9, emit_d)])
    send(second_pack, 2)
    for k, offsets in enumerate(rounds):
        pl.semaphore_wait(known_sem.at[k], heard(offsets))
        if k + 1 < len(rounds):
            greet(known_sem.at[k + 1], rounds[k + 1])

    spread(0, collect(first_sums))
    finish(first_pack, 0)
    each_right(lambda c: c.wait_send(), 1)

    own_ref[1] = jnp.where(own16, turn(state_ref[1, 32 : 32 + cols, :], -16), 0.0)
    receive(second_pack, 2)
    pipeline(early_stages(second_pack))
    m0, m1, alpha0 = step["m0"], step["m1"], step["alpha0"]
    spread(1, collect(dots))
    finish(second_pack, 2)
    all_red(0).wait_send()

    def emit_h(slot, o, e, t):
        w3 = jnp.where(own32, fold4(t, 0, 0, 1, 1) + smooth(1, o + 32, e + 32), 0.0)
        w3 = turn(w3, -16)
        own_ref[5, o:e, :] = own_ref[3, o:e, :] - alpha0 * w3

    pipeline(three_stages(second_pack, True) + [Stage(1, 2, n_in - 96, 9, emit_h)])

    def upright(k):
        return jnp.concatenate(
            [own_ref[k, j : j + LANES, :].T[16 : 16 + rows] for j in range(0, cols, LANES)], axis=1
        )

    shared_ref[...] = upright(6)
    for at, k in enumerate((1, 2, 3, 4, 5)):
        upright_ref[at] = upright(k)

    rr1, r1q, r1w, ww, qq, qw, qw2, ww2, qaq = gather(1, SUMS)
    beta0 = rr1 / m0
    alpha1 = rr1 / (r1q + beta0 * (2.0 * r1w + beta0 * m1))
    both = alpha1 * beta0
    rr2 = rr1 - 2.0 * alpha1 * (r1q + beta0 * r1w) + alpha1 * alpha1 * (
        qq + beta0 * (2.0 * qw + beta0 * ww)
    )
    beta1 = rr2 / rr1
    r2ar2 = (
        r1q + alpha1 * alpha1 * qaq + both * both * ww2
        - 2.0 * alpha1 * qq - 2.0 * both * qw + 2.0 * alpha1 * both * qw2
    )
    alpha2 = rr2 / (r2ar2 - beta1 * rr2 / alpha1)
    t_r0 = alpha0 + both + alpha2 * beta1 * beta0
    t_r1 = alpha1 + alpha2 * (1.0 + beta1)
    t_q, t_w1 = -alpha2 * alpha1, -alpha2 * both
    s_q, s_w1 = -alpha1 - alpha2 * (1.0 + beta1), -both - alpha2 * beta1 * beta0
    s_aq, s_w2 = alpha2 * alpha1, alpha2 * both
    r0, w1, w2, q, aq = (upright_ref[k] for k in range(5))
    template_ref[...] = guess_ref[...] + t_r0 * r0 + (t_r1 - 1.0) * shared_ref[...] + t_q * q + t_w1 * w1
    residual_ref[...] = s_q * q + s_w1 * w1 + s_aq * aq + s_w2 * w2
    all_red(1).wait_send()


def on_device(n_row, n_col, right_side, initial_guess, kernel):
    rows, cols = right_side.shape
    count = n_row * n_col
    shape = pltpu.VMEM((rows, cols), jnp.float32)
    f32, bf16 = jnp.float32, jnp.bfloat16
    tall = cols + 2 * rows
    packs = [pltpu.VMEM((3, cols // 16 + 2 * (rows // 16), 8, LANES), f32) for _ in range(2)]
    packs.insert(1, pltpu.VMEM((6, cols // 32 + 2, 8, LANES), f32))
    template, residual, shared = pl.pallas_call(
        functools.partial(body, n_row, n_col),
        out_shape=(shape,) * 3,
        in_specs=[pl.BlockSpec(memory_space=pl.ANY)] * 3,
        out_specs=[pl.BlockSpec(memory_space=pltpu.VMEM)] * 3,
        scratch_shapes=[
            pltpu.VMEM((rows, cols), f32),
            pltpu.VMEM((rows, cols), f32),
            pltpu.VMEM(kernel.shape, f32),
            *packs,
            pltpu.VMEM((2, LANES, LANES), f32),
            pltpu.VMEM((2, 2, 2 * LANES, 2 * LANES), bf16),
            pltpu.VMEM((2, 5, tall, LANES), bf16),
            pltpu.VMEM((2, 5, tall, LANES), bf16),
            pltpu.VMEM((2, 2, 5, tall, LANES), f32),
            pltpu.VMEM((2, 5, tall, LANES), f32),
            pltpu.VMEM((2, tall, LANES), f32),
            pltpu.VMEM((cols // 32 + 2, 4, 8, LANES), f32),
            pltpu.VMEM((7, cols, LANES), f32),
            pltpu.VMEM((5, rows, cols), f32),
            pltpu.VMEM((2, count, 1, LANES), f32),
            pltpu.SemaphoreType.DMA((3,)),
            pltpu.SemaphoreType.DMA((3, len(DIRECTIONS))),
            pltpu.SemaphoreType.DMA((3, len(DIRECTIONS))),
            pltpu.SemaphoreType.DMA((2,)),
            pltpu.SemaphoreType.DMA((2,)),
            pltpu.SemaphoreType.REGULAR((len(greetings(n_row, n_col)),)),
        ],
        compiler_params=pltpu.CompilerParams(collective_id=0, has_side_effects=True),
    )(right_side, initial_guess, kernel)
    return template + shared, residual + shared


def solution(mesh):
    placed = (P("row", "col"), P("row", "col"), P())
    return jax.shard_map(
        functools.partial(on_device, mesh.shape["row"], mesh.shape["col"]),
        mesh=mesh,
        in_specs=placed,
        out_specs=(P("row", "col"), P("row", "col")),
        check_vma=False,
    )
```
